8 devices in a mesh: inst: 1 (over z), dev: 2 (over y), side: 4 (over x, core).
Axes of the slice: x: 2, y: 2, z: 1, core: 2. Of those that a mesh axis runs over, the one named last changes fastest.
Arguments:
- hidden: bfloat16 [512, 3584], P(('inst', 'dev'))
- cache_len: int32 [512], P(('inst', 'dev'))
- k_cache: bfloat16 [3, 512, 4, 64, 128], P(None, ('inst', 'dev'))
- v_cache: bfloat16 [3, 512, 4, 64, 128], P(None, ('inst', 'dev'))
- w_q: bfloat16 [3, 3584, 3584], replicated
- w_kv: bfloat16 [3, 3584, 1024], replicated
- w_o: bfloat16 [3, 3584, 3584], replicated
- attn_gain: float32 [3, 3584], replicated
- ffn_gain: float32 [3, 3584], replicated
- w_gate: bfloat16 [3, 3584, 18944], P(None, None, 'dev')
- w_up: bfloat16 [3, 3584, 18944], P(None, None, 'dev')
- w_down: bfloat16 [3, 18944, 3584], P(None, 'dev')
Outputs:
- output: bfloat16 [512, 3584], P(('inst', 'dev', 'side'))
All inputs are finite; a program needn't handle non-finite values.
Results may differ from the reference program's by a relative error of at most 0.02.
Values are sent between devices in bfloat16 or wider.
A program may use at most 3.5 GiB of HBM per device.

```python
import math
import jax
import jax.numpy as jnp
from jax import lax

D = 3584
FF = 18944
HEADS = 28
KV_HEADS = 4
HEAD = 128
SEQ = 64
LAYERS = 3
BATCH = 512

EPS = 1e-5
ROPE_BASE = 10000.0
KEY_STD = math.sqrt(1.5 * math.log(SEQ))
GROUP = HEADS // KV_HEADS


def setup_inputs(seed: int = 0, part: int = 0) -> dict:
    base_key = jax.random.key(seed)
    part_key = jax.random.fold_in(base_key, part)
    shared = jax.random.split(base_key, 8)
    local = jax.random.split(part_key, 6)
    hidden = jax.random.normal(local[0], (BATCH, D), jnp.float32)
    cache_len = jax.random.randint(local[1], (BATCH,), 1, SEQ + 1, dtype=jnp.int32)
    cache_len = cache_len.at[0].set(SEQ).at[1].set(1)
    cache_shape = (LAYERS, BATCH, KV_HEADS, SEQ, HEAD)
    mean_shape = (LAYERS, BATCH, KV_HEADS, 1, HEAD)
    pos_ramp = (2.0 * jnp.arange(SEQ, dtype=jnp.float32) / SEQ - 1.0).reshape(1, 1, 1, SEQ, 1)
    k_cache = KEY_STD * jax.random.normal(local[2], cache_shape, jnp.float32)
    v_cache = (jax.random.normal(local[3], cache_shape, jnp.float32)
               + 0.7 * jax.random.normal(local[4], mean_shape, jnp.float32)
               + 0.7 * pos_ramp * jax.random.normal(local[5], mean_shape, jnp.float32))
    kv_cols = KV_HEADS * HEAD
    col_scale = jnp.concatenate([jnp.full((kv_cols,), KEY_STD, jnp.float32), jnp.full((kv_cols,), 2.0, jnp.float32)])
    w_q = jax.random.normal(shared[0], (LAYERS, D, HEADS * HEAD), jnp.float32) * D ** -0.5
    w_kv = jax.random.normal(shared[1], (LAYERS, D, 2 * kv_cols), jnp.float32) * (D ** -0.5) * col_scale
    w_o = jax.random.normal(shared[2], (LAYERS, HEADS * HEAD, D), jnp.float32) * (HEADS * HEAD) ** -0.5
    attn_gain = jax.random.uniform(shared[3], (LAYERS, D), jnp.float32, 0.5, 1.5)
    ffn_gain = jax.random.uniform(shared[4], (LAYERS, D), jnp.float32, 0.5, 1.5)
    w_gate = jax.random.normal(shared[5], (LAYERS, D, FF), jnp.float32) * D ** -0.5
    w_up = jax.random.normal(shared[6], (LAYERS, D, FF), jnp.float32) * D ** -0.5
    w_down = jax.random.normal(shared[7], (LAYERS, FF, D), jnp.float32) * (1.5 * FF ** -0.5)
    return {
        'hidden': hidden.astype(jnp.bfloat16),
        'cache_len': cache_len,
        'k_cache': k_cache.astype(jnp.bfloat16),
        'v_cache': v_cache.astype(jnp.bfloat16),
        'w_q': w_q.astype(jnp.bfloat16),
        'w_kv': w_kv.astype(jnp.bfloat16),
        'w_o': w_o.astype(jnp.bfloat16),
        'attn_gain': attn_gain,
        'ffn_gain': ffn_gain,
        'w_gate': w_gate.astype(jnp.bfloat16),
        'w_up': w_up.astype(jnp.bfloat16),
        'w_down': w_down.astype(jnp.bfloat16),
    }


def rms_norm(rows, gain):
    rows_f = rows.astype(jnp.float32)
    inv_rms = lax.rsqrt(jnp.mean(rows_f * rows_f, axis=-1, keepdims=True) + EPS)
    return (rows_f * inv_rms * gain).astype(jnp.bfloat16)


def rotary(vecs, positions):
    half_dim = vecs.shape[-1] // 2
    freqs = ROPE_BASE ** (-jnp.arange(half_dim, dtype=jnp.float32) / half_dim)
    angle = positions.astype(jnp.float32)[:, None, None] * freqs
    cos_part = jnp.cos(angle)
    sin_part = jnp.sin(angle)
    first = vecs[..., :half_dim]
    second = vecs[..., half_dim:]
    return jnp.concatenate([first * cos_part - second * sin_part, second * cos_part + first * sin_part], axis=-1)


def attend_one(operands):
    q_row, k_new, v_new, k_seq, v_seq, length = operands
    scale = HEAD ** -0.5
    q_f = q_row.astype(jnp.float32)
    scores = jnp.einsum('kgd,ksd->kgs', q_f, k_seq.astype(jnp.float32)) * scale
    valid = jnp.arange(SEQ)[None, None, :] < length
    scores = jnp.where(valid, scores, -1e30)
    self_score = jnp.einsum('kgd,kd->kg', q_f, k_new.astype(jnp.float32)) * scale
    row_max = jnp.maximum(jnp.max(scores, axis=-1), self_score)
    exp_scores = jnp.exp(scores - row_max[..., None])
    self_exp = jnp.exp(self_score - row_max)
    total_exp = jnp.sum(exp_scores, axis=-1) + self_exp
    mixed = jnp.einsum('kgs,ksd->kgd', exp_scores.astype(jnp.bfloat16).astype(jnp.float32), v_seq.astype(jnp.float32))
    mixed = mixed + self_exp.astype(jnp.bfloat16).astype(jnp.float32)[..., None] * v_new.astype(jnp.float32)[:, None, :]
    return (mixed / total_exp[..., None]).astype(jnp.bfloat16)


def reference(hidden, cache_len, k_cache, v_cache, w_q, w_kv, w_o, attn_gain, ffn_gain, w_gate, w_up, w_down):
    def layer_step(x_cur, per_layer):
        q_weight, kv_weight, o_weight, gain_attn, gain_ffn, gate_weight, up_weight, down_weight, k_layer, v_layer = per_layer
        normed = rms_norm(x_cur, gain_attn)
        q_all = jnp.dot(normed, q_weight, preferred_element_type=jnp.float32).reshape(BATCH, HEADS, HEAD)
        kv_all = jnp.dot(normed, kv_weight, preferred_element_type=jnp.float32).reshape(BATCH, 2, KV_HEADS, HEAD)
        q_rows = rotary(q_all, cache_len).astype(jnp.bfloat16).reshape(BATCH, KV_HEADS, GROUP, HEAD)
        k_new = rotary(kv_all[:, 0], cache_len).astype(jnp.bfloat16)
        v_new = kv_all[:, 1].astype(jnp.bfloat16)
        mixed = lax.map(attend_one, (q_rows, k_new, v_new, k_layer, v_layer, cache_len))
        attn_out = jnp.dot(mixed.reshape(BATCH, HEADS * HEAD), o_weight, preferred_element_type=jnp.float32)
        x_mid = (x_cur.astype(jnp.float32) + attn_out).astype(jnp.bfloat16)
        h_rows = rms_norm(x_mid, gain_ffn)
        gate = jnp.dot(h_rows, gate_weight, preferred_element_type=jnp.float32)
        up_proj = jnp.dot(h_rows, up_weight, preferred_element_type=jnp.float32)
        act_rows = (jax.nn.silu(gate) * up_proj).astype(jnp.bfloat16)
        y_rows = jnp.dot(act_rows, down_weight, preferred_element_type=jnp.float32).astype(jnp.bfloat16)
        x_next = (x_mid.astype(jnp.float32) + y_rows.astype(jnp.float32)).astype(jnp.bfloat16)
        return x_next, None

    x_out, _ = lax.scan(layer_step, hidden, (w_q, w_kv, w_o, attn_gain, ffn_gain, w_gate, w_up, w_down, k_cache, v_cache))
    return x_out
```

```python
import functools

import jax
import jax.numpy as jnp
from jax import lax
from jax.experimental import pallas as pl
from jax.experimental.pallas import tpu as pltpu
from jax.sharding import PartitionSpec as P

EPS = 1e-5
ROPE_BASE = 10000.0
MESH = pl.DeviceIdType.MESH
F32 = jnp.float32
BF16 = jnp.bfloat16

TN = 256
NS = 16
GS = 8
CS = 32
GU_UNROLL = 4
DN_UNROLL = 2


def dot(lhs, rhs):
    return jnp.dot(lhs, rhs, preferred_element_type=F32)


def kernel(dims, cos_ref, sin_ref, len_ref, ag_ref, fg_ref, hid, kc, vc, wq, wkv, wo, wg, wu, wd, out,
           ring, xc, x1, h, qf, kn, vn, of, oa, u, yp, dr, yr, kb, vb,
           ring_sem, cache_sem, in_sem, o_send, o_recv, xp_send, xp_recv, xy_send, xy_recv, xf_send, xf_recv,
           d_send, d_recv, y_send, y_recv, e_send, e_recv):
    n_layers, d_model, ff, heads, kv_heads, head, seq = dims
    half_d = d_model // 2
    nch = d_model // TN
    nq = half_d // TN
    rows = xc.shape[2]
    ngu = ff // 128
    group = heads // kv_heads
    r_kv = nq
    r_o = nq + 2
    r_gu = r_o + nq
    r_dn = r_gu + ngu
    tiles = r_dn + nch

    side = lax.axis_index("side")
    dev = lax.axis_index("dev")
    c = lax.rem(side, 2)
    oc = 1 - c
    base = (side - c) * rows
    pair = {"side": side + 1 - 2 * c}
    ypeer = {"dev": 1 - dev}

    barrier = pltpu.get_barrier_semaphore()
    pl.semaphore_signal(barrier, inc=1, device_id=pair, device_id_type=MESH)
    pl.semaphore_signal(barrier, inc=1, device_id=ypeer, device_id_type=MESH)

    def rcopy(src, dst, ssem, rsem, where):
        return pltpu.make_async_remote_copy(
            src_ref=src, dst_ref=dst, send_sem=ssem, recv_sem=rsem, device_id=where, device_id_type=MESH)

    def al(v, m):
        return pl.multiple_of(v, m)

    def slot_of(layer, r):
        return lax.rem(layer * tiles + r, NS)

    def issue(layer, r):
        slot = slot_of(layer, r)
        sem = ring_sem.at[slot]
        top = ring.at[slot, pl.ds(0, d_model)]

        @pl.when(r < r_kv)
        def _():
            pltpu.make_async_copy(wq.at[layer, :, pl.ds(al(c * half_d + r * TN, TN), TN)], top, sem).start()

        @pl.when((r >= r_kv) & (r < r_o))
        def _():
            col = (r - r_kv) * (2 * TN) + c * TN
            pltpu.make_async_copy(wkv.at[layer, :, pl.ds(al(col, TN), TN)], top, sem).start()

        @pl.when((r >= r_o) & (r < r_gu))
        def _():
            col = c * half_d + (r - r_o) * TN
            pltpu.make_async_copy(wo.at[layer, :, pl.ds(al(col, TN), TN)], top, sem).start()

        @pl.when((r >= r_gu) & (r < r_dn))
        def _():
            col = al(c * ff + (r - r_gu) * 128, 128)
            pltpu.make_async_copy(
                wg.at[layer, :, pl.ds(col, 128)], ring.at[slot, pl.ds(0, d_model), pl.ds(0, 128)], sem).start()
            pltpu.make_async_copy(
                wu.at[layer, :, pl.ds(col, 128)], ring.at[slot, pl.ds(0, d_model), pl.ds(128, 128)], sem).start()

        @pl.when(r >= r_dn)
        def _():
            pltpu.make_async_copy(
                wd.at[layer, pl.ds(al(c * ff, 128), ff), pl.ds(al((r - r_dn) * TN, TN), TN)], ring.at[slot], sem).start()

    def release(layer, r):
        nxt = r + NS
        wrap = (nxt >= tiles).astype(jnp.int32) if not isinstance(nxt, int) else int(nxt >= tiles)
        lay = layer + wrap
        rr = nxt - tiles * wrap

        @pl.when(lay < n_layers)
        def _():
            issue(lay, rr)

    def wait_top(layer, r):
        slot = slot_of(layer, r)
        pltpu.make_async_copy(wq.at[0, :, pl.ds(0, TN)], ring.at[slot, pl.ds(0, d_model)], ring_sem.at[slot]).wait()
        return slot

    def wait_full(layer, r):
        slot = slot_of(layer, r)
        pltpu.make_async_copy(wd.at[0, pl.ds(0, ff), pl.ds(0, TN)], ring.at[slot], ring_sem.at[slot]).wait()
        return slot

    def cache_copies(layer, ch):
        slot = ch % 2 if isinstance(ch, int) else lax.rem(ch, 2)
        src = pl.ds(al(base + ch * CS, CS), CS)
        hd = pl.ds(c * 2, 2)
        return (pltpu.make_async_copy(kc.at[layer, src, hd], kb.at[slot], cache_sem.at[slot, 0]),
                pltpu.make_async_copy(vc.at[layer, src, hd], vb.at[slot], cache_sem.at[slot, 1]))

    def norm_rows(src, chip, gain, layer, dst_row):
        for k in range(2):
            for part in range(rows // 32):
                rs = slice(part * 32, part * 32 + 32)
                total = jnp.zeros((32, TN), F32)
                for j in range(nch):
                    v = (src[chip, j, k, rs, :] if chip is not None else src[j, k, rs, :]).astype(F32)
                    total = total + v * v
                inv = lax.rsqrt(jnp.sum(total, axis=-1, keepdims=True) * (1.0 / d_model) + EPS)
                r0 = dst_row + k * rows + part * 32
                for j in range(nch):
                    v = (src[chip, j, k, rs, :] if chip is not None else src[j, k, rs, :]).astype(F32)
                    h[r0:r0 + 32, j * TN:(j + 1) * TN] = (v * inv * gain[layer, j]).astype(BF16)

    for r in range(NS):
        issue(0, jnp.int32(r))
    for ch in range(2):
        for cp in cache_copies(0, ch):
            cp.start()
    for j in range(nch):
        for k in range(2):
            pltpu.make_async_copy(
                hid.at[pl.ds(al(base + k * rows, rows), rows), pl.ds(j * TN, TN)], xc.at[j, k], in_sem.at[j, k]).start()
    for j in range(nch):
        for k in range(2):
            pltpu.make_async_copy(hid.at[pl.ds(0, rows), pl.ds(0, TN)], xc.at[j, k], in_sem.at[j, k]).wait()
    pl.semaphore_wait(barrier, 2)

    col = lax.broadcasted_iota(jnp.int32, (GS, GS * seq), 1)
    row = lax.broadcasted_iota(jnp.int32, (GS, GS * seq), 0)
    own_keys = lax.shift_right_logical(col, seq.bit_length() - 1) == row
    key_pos = jnp.bitwise_and(col, seq - 1)
    scale = head ** -0.5

    def layer_body(layer, carry):
        not_last = layer + 1 < n_layers

        norm_rows(xc, None, ag_ref, layer, 0)
        cos_v = cos_ref[...]
        sin_v = sin_ref[...]

        def rope(v):
            return (v * cos_v + pltpu.roll(v, head // 2, 1) * sin_v).astype(BF16).astype(F32)

        for g0 in range(0, r_o, 3):
            rs = list(range(g0, min(g0 + 3, r_o)))
            slots = [wait_top(layer, r) for r in rs]
            for r, slot in zip(rs, slots):
                y = dot(h[:2 * rows, :], ring[slot, :d_model, :])
                for k in range(2):
                    part = y[:, k * head:(k + 1) * head]
                    if r < r_kv:
                        qf[r * 2 + k] = rope(part)
                    elif r == r_kv:
                        kn[k] = rope(part)
                    else:
                        vn[k] = part.astype(BF16).astype(F32)
            for r in rs:
                release(layer, r)

        def chunk_body(ch, carry):
            slot = lax.rem(ch, 2)
            for cp in cache_copies(layer, ch):
                cp.wait()
            for gi in range(CS // GS):
                r0 = al(ch * CS + gi * GS, GS)
                valid = own_keys & (key_pos < len_ref[pl.ds(r0, GS), :])
                for k in range(2):
                    q = qf[k * group:(k + 1) * group, pl.ds(r0, GS), :]
                    keys = kb[slot, gi * GS:(gi + 1) * GS, k].reshape(GS * seq, head)
                    vals = vb[slot, gi * GS:(gi + 1) * GS, k].reshape(GS * seq, head)
                    sc = lax.dot_general(q.reshape(group * GS, head).astype(BF16), keys, (((1,), (1,)), ((), ())),
                                         preferred_element_type=F32)
                    sc = sc.reshape(group, GS, GS * seq) * scale
                    sc = jnp.where(valid[None], sc, -1e30)
                    k_new = kn[k, pl.ds(r0, GS), :]
                    v_new = vn[k, pl.ds(r0, GS), :]
                    self_sc = jnp.sum(q * k_new[None], axis=-1, keepdims=True) * scale
                    top = jnp.maximum(jnp.max(sc, axis=-1, keepdims=True), self_sc)
                    e = jnp.exp(sc - top)
                    self_e = jnp.exp(self_sc - top)
                    total = jnp.sum(e, axis=-1, keepdims=True) + self_e
                    mix = dot(e.reshape(group * GS, GS * seq).astype(BF16), vals).reshape(group, GS, head)
                    mix = mix + self_e.astype(BF16).astype(F32) * v_new[None]
                    of[k * group:(k + 1) * group, gi * GS:(gi + 1) * GS, :] = mix / total
            rr = pl.ds(al(ch * CS, CS), CS)
            for hh in range(heads // 2):
                oa[c, rr, hh * head:(hh + 1) * head] = of[hh].astype(BF16)
            rcopy(oa.at[c, rr], oa.at[c, rr], o_send.at[ch], o_recv.at[ch], pair).start()
            nxt = ch + 2

            @pl.when(nxt < n_chunks)
            def _():
                for cp in cache_copies(layer, nxt):
                    cp.start()

            @pl.when((nxt >= n_chunks) & not_last)
            def _():
                for cp in cache_copies(layer + 1, nxt - n_chunks):
                    cp.start()

            return carry

        n_chunks = 2 * rows // CS
        lax.fori_loop(0, n_chunks, chunk_body, 0)
        for ch in range(n_chunks):
            rr = pl.ds(ch * CS, CS)
            rcopy(oa.at[oc, rr], oa.at[oc, rr], o_send.at[ch], o_recv.at[ch], pair).wait_recv()

        for g0 in range(0, nq, 2):
            js = list(range(g0, min(g0 + 2, nq)))
            slots = [wait_top(layer, r_o + j) for j in js]
            for j, slot in zip(js, slots):
                acc = dot(oa[0], ring[slot, :half_d, :]) + dot(oa[1], ring[slot, half_d:d_model, :])
                acc = acc + xc[c * nq + j].reshape(2 * rows, TN).astype(F32)
                x1[0, c * nq + j] = acc.astype(BF16).reshape(2, rows, TN)
            for j in js:
                mine = c * nq + j
                rcopy(x1.at[0, mine], x1.at[1, mine], xy_send.at[j], xy_recv.at[j], ypeer).start()
                rcopy(x1.at[0, mine], x1.at[0, mine], xp_send.at[j], xp_recv.at[j], pair).start()
                release(layer, r_o + j)
        for j in range(nq):
            theirs = oc * nq + j
            rcopy(x1.at[0, theirs], x1.at[0, theirs], xp_send.at[j], xp_recv.at[j], pair).wait_recv()
        norm_rows(x1, 0, fg_ref, layer, 0)
        for j in range(nq):
            mine = c * nq + j
            rcopy(x1.at[1, mine], x1.at[1, mine], xy_send.at[j], xy_recv.at[j], ypeer).wait_recv()
            rcopy(x1.at[1, mine], x1.at[1, mine], xf_send.at[j], xf_recv.at[j], pair).start()
        for j in range(nq):
            theirs = oc * nq + j
            rcopy(x1.at[1, theirs], x1.at[1, theirs], xf_send.at[j], xf_recv.at[j], pair).wait_recv()
        norm_rows(x1, 1, fg_ref, layer, 2 * rows)

        def gate_up(first, count):
            slots = [wait_top(layer, r_gu + first + i) for i in range(count)]
            for i, slot in enumerate(slots):
                y = dot(h[...], ring[slot, :d_model, :])
                gate = y[:, :128]
                act = gate * (1.0 / (1.0 + jnp.exp(-gate))) * y[:, 128:]
                u[:, pl.ds(al((first + i) * 128, 128), 128)] = act.astype(BF16)
            for i in range(count):
                release(layer, r_gu + first + i)

        full = ngu // GU_UNROLL

        def gu_body(i, carry):
            gate_up(i * GU_UNROLL, GU_UNROLL)
            return carry

        lax.fori_loop(0, full, gu_body, 0)
        if ngu % GU_UNROLL:
            gate_up(full * GU_UNROLL, ngu % GU_UNROLL)

        for j in range(nq):
            mine = c * nq + j
            rcopy(x1.at[1, mine], x1.at[1, mine], xf_send.at[j], xf_recv.at[j], pair).wait_send()

        def pair_sum(j):
            rcopy(yp.at[j, oc], dr.at[j], d_send.at[j], d_recv.at[j], pair).wait_recv()
            yp[j, c, 1] = yp[j, c, 1] + dr[j, 1]
            rcopy(yp.at[j, c, 1], yr.at[j], y_send.at[j], y_recv.at[j], ypeer).start()

        def down_body(i, carry):
            j0 = i * DN_UNROLL
            slots = [wait_full(layer, r_dn + j0 + k) for k in range(DN_UNROLL)]
            for k, slot in enumerate(slots):
                y = dot(u[...], ring[slot])
                for chip in range(2):
                    for core in range(2):
                        r0 = (chip * 2 + core) * rows
                        yp[j0 + k, core, chip] = y[r0:r0 + rows, :]
            for k in range(DN_UNROLL):
                rcopy(yp.at[j0 + k, oc], dr.at[j0 + k], d_send.at[j0 + k], d_recv.at[j0 + k], pair).start()
                release(layer, r_dn + j0 + k)

            @pl.when(i > 0)
            def _():
                for k in range(DN_UNROLL):
                    pair_sum(j0 - DN_UNROLL + k)

            return carry

        lax.fori_loop(0, nch // DN_UNROLL, down_body, 0)
        for k in range(DN_UNROLL):
            pair_sum(nch - DN_UNROLL + k)

        def finish(j, carry):
            rcopy(yp.at[j, c, 1], yr.at[j], y_send.at[j], y_recv.at[j], ypeer).wait_recv()
            y = (yp[j, c, 0] + dr[j, 0] + yr[j]).astype(BF16).astype(F32)
            xc[j, c] = (x1[0, j, c].astype(F32) + y).astype(BF16)

            @pl.when(not_last)
            def _():
                rcopy(xc.at[j, c], xc.at[j, c], e_send.at[j], e_recv.at[j], pair).start()

            @pl.when(jnp.logical_not(not_last))
            def _():
                pltpu.make_async_copy(xc.at[j, c], out.at[:, pl.ds(al(j * TN, TN), TN)], e_send.at[j]).start()

            return carry

        lax.fori_loop(0, nch, finish, 0)

        for ch in range(n_chunks):
            rr = pl.ds(ch * CS, CS)
            rcopy(oa.at[c, rr], oa.at[c, rr], o_send.at[ch], o_recv.at[ch], pair).wait_send()
        for j in range(nq):
            mine = c * nq + j
            rcopy(x1.at[0, mine], x1.at[1, mine], xy_send.at[j], xy_recv.at[j], ypeer).wait_send()
            rcopy(x1.at[0, mine], x1.at[0, mine], xp_send.at[j], xp_recv.at[j], pair).wait_send()
        for j in range(nch):
            rcopy(yp.at[j, oc], dr.at[j], d_send.at[j], d_recv.at[j], pair).wait_send()
            rcopy(yp.at[j, c, 1], yr.at[j], y_send.at[j], y_recv.at[j], ypeer).wait_send()

        @pl.when(not_last)
        def _():
            for j in range(nch):
                rcopy(xc.at[j, oc], xc.at[j, oc], e_send.at[j], e_recv.at[j], pair).wait_recv()
                rcopy(xc.at[j, c], xc.at[j, c], e_send.at[j], e_recv.at[j], pair).wait_send()

        @pl.when(jnp.logical_not(not_last))
        def _():
            for j in range(nch):
                pltpu.make_async_copy(xc.at[j, c], out.at[:, pl.ds(j * TN, TN)], e_send.at[j]).wait()

        return carry

    lax.fori_loop(0, n_layers, layer_body, 0)


def solution(mesh):
    batch_axes = ('inst', 'dev')
    in_specs = (
        P(batch_axes, None),
        P(batch_axes),
        P(None, batch_axes, None, None, None),
        P(None, batch_axes, None, None, None),
        P(), P(), P(), P(), P(),
        P(None, None, 'dev'),
        P(None, None, 'dev'),
        P(None, 'dev', None),
    )
    out_specs = P(('inst', 'dev', 'side'), None)
    n_side = mesh.shape['side']

    def device_fn(hidden, cache_len, k_cache, v_cache, w_q, w_kv, w_o, attn_gain, ffn_gain, w_gate, w_up, w_down):
        n_layers, d_model, _ = w_q.shape
        kv_heads, seq, head = k_cache.shape[2:]
        heads = w_q.shape[2] // head
        rows = hidden.shape[0] // n_side
        ff = w_gate.shape[2] // 2
        nch = d_model // TN
        nq = nch // 2
        side = lax.axis_index('side')
        lengths = lax.dynamic_slice_in_dim(cache_len, (side // 2) * (2 * rows), 2 * rows)
        half_dim = head // 2
        freqs = ROPE_BASE ** (-jnp.arange(half_dim, dtype=F32) / half_dim)
        angle = lengths.astype(F32)[:, None] * jnp.concatenate([freqs, freqs])
        sign = jnp.where(jnp.arange(head) < half_dim, -1.0, 1.0).astype(F32)
        cos_tab = jnp.cos(angle)
        sin_tab = jnp.sin(angle) * sign
        len_tab = jnp.broadcast_to(lengths[:, None], (2 * rows, GS * seq))
        gains = [g.reshape(n_layers, nch, 1, TN) for g in (attn_gain, ffn_gain)]
        dims = (n_layers, d_model, ff, heads, kv_heads, head, seq)
        vmem = pl.BlockSpec(memory_space=pltpu.VMEM)
        hbm = pl.BlockSpec(memory_space=pl.ANY)
        dma = pltpu.SemaphoreType.DMA
        n_chunks = 2 * rows // CS
        return pl.pallas_call(
            functools.partial(kernel, dims),
            name='decode_layers',
            out_shape=jax.ShapeDtypeStruct((rows, d_model), BF16),
            in_specs=[vmem] * 5 + [hbm] * 9,
            out_specs=hbm,
            scratch_shapes=[
                pltpu.VMEM((NS, ff, TN), BF16),
                pltpu.VMEM((nch, 2, rows, TN), BF16),
                pltpu.VMEM((2, nch, 2, rows, TN), BF16),
                pltpu.VMEM((4 * rows, d_model), BF16),
                pltpu.VMEM((heads // 2, 2 * rows, head), F32),
                pltpu.VMEM((2, 2 * rows, head), F32),
                pltpu.VMEM((2, 2 * rows, head), F32),
                pltpu.VMEM((heads // 2, CS, head), F32),
                pltpu.VMEM((2, 2 * rows, d_model // 2), BF16),
                pltpu.VMEM((4 * rows, ff), BF16),
                pltpu.VMEM((nch, 2, 2, rows, TN), F32),
                pltpu.VMEM((nch, 2, rows, TN), F32),
                pltpu.VMEM((nch, rows, TN), F32),
                pltpu.VMEM((2, CS, 2, seq, head), BF16),
                pltpu.VMEM((2, CS, 2, seq, head), BF16),
                dma((NS,)), dma((2, 2)), dma((nch, 2)),
                dma((n_chunks,)), dma((n_chunks,)),
                dma((nq,)), dma((nq,)), dma((nq,)), dma((nq,)), dma((nq,)), dma((nq,)),
                dma((nch,)), dma((nch,)), dma((nch,)), dma((nch,)), dma((nch,)), dma((nch,)),
            ],
            compiler_params=pltpu.CompilerParams(
                collective_id=0, has_side_effects=True, vmem_limit_bytes=67043328),
        )(cos_tab, sin_tab, len_tab, *gains, hidden, k_cache, v_cache, w_q, w_kv, w_o, w_gate, w_up, w_down)

    return jax.shard_map(device_fn, mesh=mesh, in_specs=in_specs, out_specs=out_specs, check_vma=False)
```

```python
import functools

import jax
import jax.numpy as jnp
import numpy as np
from jax import lax
from jax.experimental import pallas as pl
from jax.experimental.pallas import tpu as pltpu
from jax.sharding import PartitionSpec as P

EPS = 1e-5
ROPE_BASE = 10000.0
MESH = pl.DeviceIdType.MESH
F32 = jnp.float32
BF16 = jnp.bfloat16

TN = 256
NS = 16
GS = 8
GU = 7
DN_STEPS = (2, 2, 2, 2, 2, 2, 2)
QKV_STEPS = (4, 5)
O_STEPS = (2, 2, 3)


def spans(steps, total):
    assert sum(steps) == total
    out, at = [], 0
    for n in steps:
        out.append(list(range(at, at + n)))
        at += n
    return out


def dot(lhs, rhs):
    return jnp.dot(lhs, rhs, preferred_element_type=F32)


def kernel(dims, len_ref, freq_ref, ag_ref, fg_ref, hid, kc, vc, wq, wkv, wo, wg, wu, wd, out,
           ring, xc, x1, h, qf, kn, vn, of, oa, acc_s, u, yp, dr, yr, kb, vb, cos_t, sin_t, len_t,
           ring_sem, cache_sem, in_sem, o_send, o_recv, xp_send, xp_recv, xy_send, xy_recv, xf_send, xf_recv,
           d_send, d_recv, y_send, y_recv, e_send, e_recv):
    n_layers, d_model, ff, heads, kv_heads, head, seq = dims
    half_d = d_model // 2
    nch = d_model // TN
    nq = half_d // TN
    hr = xc.shape[3]
    ngu = ff // 128
    group = heads // kv_heads
    r_o = nq + 2
    r_gu = r_o + nq
    r_dn = r_gu + ngu
    tiles = r_dn + nch
    assert r_gu == NS

    side = lax.axis_index("side")
    dev = lax.axis_index("dev")
    c = lax.rem(side, 2)
    oc = 1 - c
    base = (side - c) * (2 * hr)
    pair = {"side": side + 1 - 2 * c}
    ypeer = {"dev": 1 - dev}

    barrier = pltpu.get_barrier_semaphore()
    pl.semaphore_signal(barrier, inc=1, device_id=pair, device_id_type=MESH)
    pl.semaphore_signal(barrier, inc=1, device_id=ypeer, device_id_type=MESH)

    def rcopy(src, dst, ssem, rsem, where):
        return pltpu.make_async_remote_copy(
            src_ref=src, dst_ref=dst, send_sem=ssem, recv_sem=rsem, device_id=where, device_id_type=MESH)

    def al(v, m):
        return pl.multiple_of(v, m)

    def slot_of(layer, r):
        return lax.rem(layer * tiles + r, NS)

    def fill_attn(layer, r):
        slot = slot_of(layer, r)
        top = ring.at[slot, pl.ds(0, d_model)]
        if r < nq:
            src = wq.at[layer, :, pl.ds(al(c * half_d + r * TN, TN), TN)]
        elif r < r_o:
            src = wkv.at[layer, :, pl.ds(al((r - nq) * (2 * TN) + c * TN, TN), TN)]
        else:
            src = wo.at[layer, :, pl.ds(al(c * half_d + (r - r_o) * TN, TN), TN)]
        pltpu.make_async_copy(src, top, ring_sem.at[slot]).start()

    def fill_gu(layer, i):
        slot = slot_of(layer, r_gu + i)
        col = al(c * ff + i * 128, 128)
        for k, w in enumerate((wg, wu)):
            pltpu.make_async_copy(
                w.at[layer, :, pl.ds(col, 128)], ring.at[slot, pl.ds(0, d_model), pl.ds(k * 128, 128)],
                ring_sem.at[slot]).start()

    def fill_dn(layer, j):
        slot = slot_of(layer, r_dn + j)
        pltpu.make_async_copy(
            wd.at[layer, pl.ds(al(c * ff, 128), ff), pl.ds(al(j * TN, TN), TN)], ring.at[slot], ring_sem.at[slot]).start()

    def wait_top(slot):
        pltpu.make_async_copy(wq.at[0, :, pl.ds(0, TN)], ring.at[slot, pl.ds(0, d_model)], ring_sem.at[slot]).wait()

    def wait_full(slot):
        pltpu.make_async_copy(wd.at[0, pl.ds(0, ff), pl.ds(0, TN)], ring.at[slot], ring_sem.at[slot]).wait()

    def cache_copies(layer, half, core):
        src = pl.ds(al(base + core * (2 * hr) + half * hr, hr), hr)
        hd = pl.ds(c * 2, 2)
        return (pltpu.make_async_copy(kc.at[layer, src, hd], kb.at[core], cache_sem.at[core, 0]),
                pltpu.make_async_copy(vc.at[layer, src, hd], vb.at[core], cache_sem.at[core, 1]))

    def norm_half(read, gain, layer, dst_row):
        for k in range(2):
            total = jnp.zeros((hr, TN), F32)
            for j in range(nch):
                v = read(j, k).astype(F32)
                total = total + v * v
            inv = lax.rsqrt(jnp.sum(total, axis=-1, keepdims=True) * (1.0 / d_model) + EPS)
            r0 = dst_row + k * hr
            for j in range(nch):
                v = read(j, k).astype(F32)
                g = gain[pl.ds(layer, 1), j * TN:(j + 1) * TN]
                h[r0:r0 + hr, j * TN:(j + 1) * TN] = (v * inv * g).astype(BF16)

    def row_copy(j, half, k):
        src = hid.at[pl.ds(al(base + (k * 2 + half) * hr, hr), hr), pl.ds(j * TN, TN)]
        return pltpu.make_async_copy(src, xc.at[j, half, k], in_sem.at[j, half, k])

    rows_in = [[(j, half, k) for j in range(nch) for k in range(2)] for half in range(2)]
    for jhk in rows_in[0]:
        row_copy(*jhk).start()
    for r in range(4):
        fill_attn(0, r)

    n_pos = 4 * hr
    lens = len_ref[pl.ds(lax.div(side, 2), 1), :].astype(F32)
    len_t[...] = jnp.broadcast_to(lens, (n_pos, n_pos)).T
    angle = len_t[:, :head] * freq_ref[...]
    lane = lax.broadcasted_iota(jnp.int32, (n_pos, head), 1)
    cos_t[...] = jnp.cos(angle)
    sin_t[...] = jnp.sin(angle) * jnp.where(lane < head // 2, -1.0, 1.0)

    for jhk in rows_in[0]:
        row_copy(*jhk).wait()
    for r in range(4, r_o):
        fill_attn(0, r)
    for core in range(2):
        for cp in cache_copies(0, 0, core):
            cp.start()
    for jhk in rows_in[1]:
        row_copy(*jhk).start()
    for r in range(r_o, r_gu):
        fill_attn(0, r)
    pl.semaphore_wait(barrier, 2)

    col = lax.broadcasted_iota(jnp.int32, (GS, GS * seq), 1)
    row = lax.broadcasted_iota(jnp.int32, (GS, GS * seq), 0)
    own_keys = lax.shift_right_logical(col, seq.bit_length() - 1) == row
    key_pos = jnp.bitwise_and(col, seq - 1).astype(F32)
    scale = head ** -0.5

    def e_copy(half, j, core):
        return rcopy(xc.at[j, half, core], xc.at[j, half, core], e_send.at[half, j], e_recv.at[half, j], pair)

    def out_copy(half, j):
        dst = out.at[pl.ds(half * hr, hr), pl.ds(al(j * TN, TN), TN)]
        return pltpu.make_async_copy(xc.at[j, half, c], dst, e_send.at[half, j])

    def y_copy(half, j):
        return rcopy(yp.at[j, c, half, 1], yr.at[half, j], y_send.at[half, j], y_recv.at[half, j], ypeer)

    def d_copy(j):
        return rcopy(yp.at[j, oc], dr.at[j], d_send.at[j], d_recv.at[j], pair)

    def finish(half, after):
        def one(j, carry):
            y_copy(half, j).wait_recv()
            y = (yp[j, c, half, 0] + dr[j, half, 0] + yr[half, j]).astype(BF16).astype(F32)
            xc[j, half, c] = (x1[0, j, half, c].astype(F32) + y).astype(BF16)
            after(j)
            return carry

        lax.fori_loop(0, nch, one, 0)

    def exchange(half):
        finish(half, lambda j: e_copy(half, j, c).start())
        for j in range(nch):
            e_copy(half, j, oc).wait_recv()
            e_copy(half, j, c).wait_send()

    def sums_sent():
        for j in range(nch):
            d_copy(j).wait_send()
            for half in range(2):
                y_copy(half, j).wait_send()

    def xy_copy(half, j):
        mine = c * nq + j
        return rcopy(x1.at[0, mine, half], x1.at[1, mine, half], xy_send.at[half, j], xy_recv.at[half, j], ypeer)

    def xp_copy(half, j, core):
        at = x1.at[0, core * nq + j, half]
        return rcopy(at, at, xp_send.at[half, j], xp_recv.at[half, j], pair)

    def xf_copy(half, j, core):
        at = x1.at[1, core * nq + j, half]
        return rcopy(at, at, xf_send.at[half, j], xf_recv.at[half, j], pair)

    def o_copy(half, core, cc):
        at = oa.at[cc, half, pl.ds(al(core * hr, hr), hr)]
        return rcopy(at, at, o_send.at[half, core], o_recv.at[half, core], pair)

    def attention_half(layer, half):
        first = half == 0

        def arrive(rs):
            @pl.when(first)
            def _():
                for r in rs:
                    wait_top(slot_of(layer, r))

        def refill(rs):
            @pl.when(jnp.logical_not(first))
            def _():
                for r in rs:
                    fill_gu(layer, r)

        with jax.named_scope("norm_a"):
            norm_half(lambda j, k: xc[j, half, k], ag_ref, layer, 0)

        def both_cores(table):
            return jnp.concatenate([table[pl.ds(al((k * 2 + half) * hr, hr), hr), :] for k in range(2)], axis=0)

        cos_v = both_cores(cos_t)
        sin_v = both_cores(sin_t)

        def rope(v):
            return (v * cos_v + pltpu.roll(v, head // 2, 1) * sin_v).astype(BF16).astype(F32)

        def qkv(r):
            y = dot(h[:2 * hr, :], ring[slot_of(layer, r), :d_model, :])
            for k in range(2):
                part = y[:, k * head:(k + 1) * head]
                if r < nq:
                    qf[r * 2 + k] = rope(part)
                elif r == nq:
                    kn[k] = rope(part)
                else:
                    vn[k] = part.astype(BF16).astype(F32)

        with jax.named_scope("qkv"):
            for rs in spans(QKV_STEPS, r_o):
                arrive(rs)
                for r in rs:
                    qkv(r)
                refill(rs)

        def core_body(core, carry):
            for cp in cache_copies(layer, half, core):
                cp.wait()
            for gi in range(hr // GS):
                r_tab = al((core * 2 + half) * hr + gi * GS, GS)
                r0 = al(core * hr + gi * GS, GS)
                n_old = len_t[pl.ds(r_tab, GS), :head]
                n_old = jnp.concatenate([n_old] * (GS * seq // head), axis=1)
                valid = own_keys & (key_pos < n_old)
                for k in range(2):
                    q = qf[k * group:(k + 1) * group, pl.ds(r0, GS), :]
                    keys = kb[core, gi * GS:(gi + 1) * GS, k].reshape(GS * seq, head)
                    vals = vb[core, gi * GS:(gi + 1) * GS, k].reshape(GS * seq, head)
                    sc = lax.dot_general(q.reshape(group * GS, head).astype(BF16), keys, (((1,), (1,)), ((), ())),
                                         preferred_element_type=F32)
                    sc = sc.reshape(group, GS, GS * seq) * scale
                    sc = jnp.where(valid[None], sc, -1e30)
                    k_new = kn[k, pl.ds(r0, GS), :]
                    v_new = vn[k, pl.ds(r0, GS), :]
                    self_sc = jnp.sum(q * k_new[None], axis=-1, keepdims=True) * scale
                    top = jnp.maximum(jnp.max(sc, axis=-1, keepdims=True), self_sc)
                    e = jnp.exp(sc - top)
                    self_e = jnp.exp(self_sc - top)
                    total = jnp.sum(e, axis=-1, keepdims=True) + self_e
                    mix = dot(e.reshape(group * GS, GS * seq).astype(BF16), vals).reshape(group, GS, head)
                    mix = mix + self_e.astype(BF16).astype(F32) * v_new[None]
                    of[k * group:(k + 1) * group, gi * GS:(gi + 1) * GS, :] = mix / total
            for hh in range(heads // 2):
                oa[c, half, pl.ds(al(core * hr, hr), hr), hh * head:(hh + 1) * head] = of[hh].astype(BF16)
            o_copy(half, core, c).start()

            @pl.when(first)
            def _():
                for cp in cache_copies(layer, 1, core):
                    cp.start()

            @pl.when(jnp.logical_not(first) & (layer + 1 < n_layers))
            def _():
                for cp in cache_copies(layer + 1, 0, core):
                    cp.start()

            return carry

        with jax.named_scope("attn"):
            lax.fori_loop(0, 2, core_body, 0)

        with jax.named_scope("w_o_own"):
            arrive(range(r_o, r_gu))
            for i in range(nq):
                w = ring[slot_of(layer, r_o + i), pl.ds(al(c * half_d, half_d), half_d), :]
                acc_s[i] = dot(oa[c, half], w) + xc[c * nq + i, half].reshape(2 * hr, TN).astype(F32)
        with jax.named_scope("o_wait"):
            @pl.when(jnp.logical_not(first))
            def _():
                for j in range(nq):
                    xy_copy(0, j).wait_recv()
                    xf_copy(0, j, c).start()

            for core in range(2):
                o_copy(half, core, oc).wait_recv()
        with jax.named_scope("w_o"):
            for js in spans(O_STEPS, nq):
                for i in js:
                    w = ring[slot_of(layer, r_o + i), pl.ds(al(oc * half_d, half_d), half_d), :]
                    acc = acc_s[i] + dot(oa[oc, half], w)
                    x1[0, c * nq + i, half] = acc.astype(BF16).reshape(2, hr, TN)
                for i in js:
                    xy_copy(half, i).start()
                    xp_copy(half, i, c).start()
                refill([r_o + i for i in js])

    def layer_body(layer, carry):
        not_last = layer + 1 < n_layers

        def half_body(half, carry):
            @pl.when((half == 1) & (layer == 0))
            def _():
                for jhk in rows_in[1]:
                    row_copy(*jhk).wait()

            @pl.when((half == 1) & (layer > 0))
            def _():
                with jax.named_scope("finish_b"):
                    exchange(1)
                    sums_sent()

            attention_half(layer, half)
            return carry

        lax.fori_loop(0, 2, half_body, 0)

        with jax.named_scope("ag_wait"):
            for half in range(2):
                for j in range(nq):
                    xp_copy(half, j, oc).wait_recv()
                norm_half(lambda j, k: x1[0, j, half, k], fg_ref, layer, half * 2 * hr)
                if half:
                    for j in range(nq):
                        xy_copy(half, j).wait_recv()
                        xf_copy(half, j, c).start()
                for j in range(nq):
                    xf_copy(half, j, oc).wait_recv()
                norm_half(lambda j, k: x1[1, j, half, k], fg_ref, layer, (2 + half) * 2 * hr)

        def gate_up(first, count, fill):
            slots = [slot_of(layer, r_gu + first + i) for i in range(count)]
            for slot in slots:
                wait_top(slot)
            for i, slot in enumerate(slots):
                y = dot(h[...], ring[slot, :d_model, :])
                gate = y[:, :128]
                act = gate * (1.0 / (1.0 + jnp.exp(-gate))) * y[:, 128:]
                u[:, pl.ds(al((first + i) * 128, 128), 128)] = act.astype(BF16)
            for i in range(count):
                fill(first + i)

        n_a = ngu - NS
        n_b = nch

        def gu_a(i, carry):
            gate_up(i * GU, GU, lambda t: fill_gu(layer, t + NS))
            return carry

        def gu_b(i, carry):
            gate_up(n_a + i * GU, GU, lambda t: fill_dn(layer, t - n_a))
            return carry

        def fill_next(t):
            @pl.when(not_last)
            def _():
                fill_attn(layer + 1, t - n_a - n_b)

        assert n_a % GU == 0 and n_b % GU == 0
        with jax.named_scope("gate_up"):
            lax.fori_loop(0, n_a // GU, gu_a, 0)
            lax.fori_loop(0, n_b // GU, gu_b, 0)
            gate_up(n_a + n_b, ngu - n_a - n_b, fill_next)

        for half in range(2):
            for j in range(nq):
                xf_copy(half, j, c).wait_send()
                xy_copy(half, j).wait_send()
                xp_copy(half, j, c).wait_send()
            for core in range(2):
                o_copy(half, core, c).wait_send()

        def pair_sum(j):
            d_copy(j).wait_recv()
            for half in range(2):
                yp[j, c, half, 1] = yp[j, c, half, 1] + dr[j, half, 1]
            y_copy(0, j).start()

        def down(js, before):
            slots = [slot_of(layer, r_dn + j) for j in js]
            for slot in slots:
                wait_full(slot)
            for j, slot in zip(js, slots):
                y = dot(u[...], ring[slot])
                for chip in range(2):
                    for half in range(2):
                        for core in range(2):
                            r0 = ((chip * 2 + half) * 2 + core) * hr
                            yp[j, core, half, chip] = y[r0:r0 + hr, :]
            for j in js:
                d_copy(j).start()

            @pl.when(not_last)
            def _():
                for j in js:
                    fill_attn(layer + 1, j + ngu - n_a - n_b)

            for j in before:
                pair_sum(j)

        with jax.named_scope("down"):
            steps = spans(DN_STEPS, nch)
            for js, before in zip(steps, [[]] + steps[:-1]):
                down(js, before)
        with jax.named_scope("pair_last"):
            for j in steps[-1]:
                pair_sum(j)
            for j in range(nch):
                y_copy(1, j).start()

        with jax.named_scope("finish_a"):
            @pl.when(not_last)
            def _():
                exchange(0)

            @pl.when(jnp.logical_not(not_last))
            def _():
                finish(0, lambda j: out_copy(0, j).start())

        return carry

    lax.fori_loop(0, n_layers, layer_body, 0)
    with jax.named_scope("finish_b"):
        finish(1, lambda j: out_copy(1, j).start())
        sums_sent()
        for half in range(2):
            for j in range(nch):
                out_copy(half, j).wait()


def solution(mesh):
    batch_axes = ('inst', 'dev')
    in_specs = (
        P(batch_axes, None),
        P(batch_axes),
        P(None, batch_axes, None, None, None),
        P(None, batch_axes, None, None, None),
        P(), P(), P(), P(), P(),
        P(None, None, 'dev'),
        P(None, None, 'dev'),
        P(None, 'dev', None),
    )
    out_specs = P(('inst', 'dev', 'side'), None)
    n_side = mesh.shape['side']

    def device_fn(hidden, cache_len, k_cache, v_cache, w_q, w_kv, w_o, attn_gain, ffn_gain, w_gate, w_up, w_down):
        n_layers, d_model, _ = w_q.shape
        kv_heads, seq, head = k_cache.shape[2:]
        heads = w_q.shape[2] // head
        rows = hidden.shape[0] // n_side
        ff = w_gate.shape[2] // 2
        nch = d_model // TN
        nq = nch // 2
        hr = rows // 2
        half_dim = head // 2
        freqs = np.float32(ROPE_BASE) ** (-np.arange(half_dim, dtype=np.float32) / np.float32(half_dim))
        freqs = jnp.asarray(np.concatenate([freqs, freqs])[None].astype(np.float32))
        lengths = cache_len.reshape(n_side // 2, 2 * rows)
        dims = (n_layers, d_model, ff, heads, kv_heads, head, seq)
        vmem = pl.BlockSpec(memory_space=pltpu.VMEM)
        hbm = pl.BlockSpec(memory_space=pl.ANY)
        dma = pltpu.SemaphoreType.DMA
        return pl.pallas_call(
            functools.partial(kernel, dims),
            name='decode_layers',
            out_shape=jax.ShapeDtypeStruct((rows, d_model), BF16),
            in_specs=[vmem] * 4 + [hbm] * 9,
            out_specs=hbm,
            scratch_shapes=[
                pltpu.VMEM((NS, ff, TN), BF16),
                pltpu.VMEM((nch, 2, 2, hr, TN), BF16),
                pltpu.VMEM((2, nch, 2, 2, hr, TN), BF16),
                pltpu.VMEM((4 * rows, d_model), BF16),
                pltpu.VMEM((heads // 2, rows, head), F32),
                pltpu.VMEM((2, rows, head), F32),
                pltpu.VMEM((2, rows, head), F32),
                pltpu.VMEM((heads // 2, hr, head), F32),
                pltpu.VMEM((2, 2, rows, d_model // 2), BF16),
                pltpu.VMEM((nq, rows, TN), F32),
                pltpu.VMEM((4 * rows, ff), BF16),
                pltpu.VMEM((nch, 2, 2, 2, hr, TN), F32),
                pltpu.VMEM((nch, 2, 2, hr, TN), F32),
                pltpu.VMEM((2, nch, hr, TN), F32),
                pltpu.VMEM((2, hr, 2, seq, head), BF16),
                pltpu.VMEM((2, hr, 2, seq, head), BF16),
                pltpu.VMEM((2 * rows, head), F32),
                pltpu.VMEM((2 * rows, head), F32),
                pltpu.VMEM((2 * rows, 2 * rows), F32),
                dma((NS,)), dma((2, 2)), dma((nch, 2, 2)),
                dma((2, 2)), dma((2, 2)),
                dma((2, nq)), dma((2, nq)), dma((2, nq)), dma((2, nq)), dma((2, nq)), dma((2, nq)),
                dma((nch,)), dma((nch,)), dma((2, nch)), dma((2, nch)), dma((2, nch)), dma((2, nch)),
            ],
            compiler_params=pltpu.CompilerParams(
                collective_id=0, has_side_effects=True, vmem_limit_bytes=67043328),
        )(lengths, freqs, attn_gain, ffn_gain, hidden, k_cache, v_cache, w_q, w_kv, w_o, w_gate, w_up, w_down)

    return jax.shard_map(device_fn, mesh=mesh, in_specs=in_specs, out_specs=out_specs, check_vma=False)
```

```python
import functools

import jax
import jax.numpy as jnp
import numpy as np
from jax import lax
from jax.experimental import pallas as pl
from jax.experimental.pallas import tpu as pltpu
from jax.sharding import PartitionSpec as P

EPS = 1e-5
ROPE_BASE = 10000.0
MESH = pl.DeviceIdType.MESH
F32 = jnp.float32
BF16 = jnp.bfloat16

TN = 256
NS = 16
GS = 8
GU = 7
DN_STEPS = (2, 2, 2, 2, 2, 2, 2)
QKV_STEPS = (4, 5)
O_STEPS = (2, 2, 3)


def spans(steps, total):
    assert sum(steps) == total
    out, at = [], 0
    for n in steps:
        out.append(list(range(at, at + n)))
        at += n
    return out


def dot(lhs, rhs):
    return jnp.dot(lhs, rhs, preferred_element_type=F32)


def kernel(dims, len_ref, freq_ref, ag_ref, fg_ref, hid, kc, vc, wq, wkv, wo, wg, wu, wd, out,
           ring, xc, x1, h, qf, kn, vn, p_s, tot_s, self_s, of, oa, acc_s, u, yp, dr, yr, kb, vb, cos_t, sin_t, len_t,
           ring_sem, cache_sem, in_sem, o_send, o_recv, xp_send, xp_recv, xy_send, xy_recv, xf_send, xf_recv,
           d_send, d_recv, y_send, y_recv, e_send, e_recv):
    n_layers, d_model, ff, heads, kv_heads, head, seq = dims
    half_d = d_model // 2
    nch = d_model // TN
    nq = half_d // TN
    hr = xc.shape[3]
    ngu = ff // 128
    group = heads // kv_heads
    r_o = nq + 2
    r_gu = r_o + nq
    r_dn = r_gu + ngu
    tiles = r_dn + nch
    assert r_gu == NS

    side = lax.axis_index("side")
    dev = lax.axis_index("dev")
    c = lax.rem(side, 2)
    oc = 1 - c
    base = (side - c) * (2 * hr)
    pair = {"side": side + 1 - 2 * c}
    ypeer = {"dev": 1 - dev}

    barrier = pltpu.get_barrier_semaphore()
    pl.semaphore_signal(barrier, inc=1, device_id=pair, device_id_type=MESH)
    pl.semaphore_signal(barrier, inc=1, device_id=ypeer, device_id_type=MESH)

    def rcopy(src, dst, ssem, rsem, where):
        return pltpu.make_async_remote_copy(
            src_ref=src, dst_ref=dst, send_sem=ssem, recv_sem=rsem, device_id=where, device_id_type=MESH)

    def al(v, m):
        return pl.multiple_of(v, m)

    def slot_of(layer, r):
        return lax.rem(layer * tiles + r, NS)

    def fill_attn(layer, r):
        slot = slot_of(layer, r)
        top = ring.at[slot, pl.ds(0, d_model)]
        if r < nq:
            src = wq.at[layer, :, pl.ds(al(c * half_d + r * TN, TN), TN)]
        elif r < r_o:
            src = wkv.at[layer, :, pl.ds(al((r - nq) * (2 * TN) + c * TN, TN), TN)]
        else:
            src = wo.at[layer, :, pl.ds(al(c * half_d + (r - r_o) * TN, TN), TN)]
        pltpu.make_async_copy(src, top, ring_sem.at[slot]).start()

    def fill_gu(layer, i):
        slot = slot_of(layer, r_gu + i)
        col = al(c * ff + i * 128, 128)
        for k, w in enumerate((wg, wu)):
            pltpu.make_async_copy(
                w.at[layer, :, pl.ds(col, 128)], ring.at[slot, pl.ds(0, d_model), pl.ds(k * 128, 128)],
                ring_sem.at[slot]).start()

    def fill_dn(layer, j):
        slot = slot_of(layer, r_dn + j)
        pltpu.make_async_copy(
            wd.at[layer, pl.ds(al(c * ff, 128), ff), pl.ds(al(j * TN, TN), TN)], ring.at[slot], ring_sem.at[slot]).start()

    def wait_top(slot):
        pltpu.make_async_copy(wq.at[0, :, pl.ds(0, TN)], ring.at[slot, pl.ds(0, d_model)], ring_sem.at[slot]).wait()

    def wait_full(slot):
        pltpu.make_async_copy(wd.at[0, pl.ds(0, ff), pl.ds(0, TN)], ring.at[slot], ring_sem.at[slot]).wait()

    def cache_copies(layer, half, core):
        src = pl.ds(al(base + core * (2 * hr) + half * hr, hr), hr)
        hd = pl.ds(c * 2, 2)
        return (pltpu.make_async_copy(kc.at[layer, src, hd], kb.at[core], cache_sem.at[core, 0]),
                pltpu.make_async_copy(vc.at[layer, src, hd], vb.at[core], cache_sem.at[core, 1]))

    def norm_half(read, gain, layer, dst_row):
        for k in range(2):
            total = jnp.zeros((hr, TN), F32)
            for j in range(nch):
                v = read(j, k).astype(F32)
                total = total + v * v
            inv = lax.rsqrt(jnp.sum(total, axis=-1, keepdims=True) * (1.0 / d_model) + EPS)
            r0 = dst_row + k * hr
            for j in range(nch):
                v = read(j, k).astype(F32)
                g = gain[pl.ds(layer, 1), j * TN:(j + 1) * TN]
                h[r0:r0 + hr, j * TN:(j + 1) * TN] = (v * inv * g).astype(BF16)

    def row_copy(j, half, k):
        src = hid.at[pl.ds(al(base + (k * 2 + half) * hr, hr), hr), pl.ds(j * TN, TN)]
        return pltpu.make_async_copy(src, xc.at[j, half, k], in_sem.at[j, half, k])

    rows_in = [[(j, half, k) for j in range(nch) for k in range(2)] for half in range(2)]
    for jhk in rows_in[0]:
        row_copy(*jhk).start()
    for r in range(4):
        fill_attn(0, r)

    n_pos = 4 * hr
    lens = len_ref[pl.ds(lax.div(side, 2), 1), :].astype(F32)
    len_t[...] = jnp.broadcast_to(lens, (n_pos, n_pos)).T
    angle = len_t[:, :head] * freq_ref[...]
    lane = lax.broadcasted_iota(jnp.int32, (n_pos, head), 1)
    cos_t[...] = jnp.cos(angle)
    sin_t[...] = jnp.sin(angle) * jnp.where(lane < head // 2, -1.0, 1.0)

    for jhk in rows_in[0]:
        row_copy(*jhk).wait()
    for r in range(4, r_o):
        fill_attn(0, r)
    for core in range(2):
        for cp in cache_copies(0, 0, core):
            cp.start()
    for jhk in rows_in[1]:
        row_copy(*jhk).start()
    for r in range(r_o, r_gu):
        fill_attn(0, r)
    pl.semaphore_wait(barrier, 2)

    col = lax.broadcasted_iota(jnp.int32, (GS, GS * seq), 1)
    row = lax.broadcasted_iota(jnp.int32, (GS, GS * seq), 0)
    own_keys = lax.shift_right_logical(col, seq.bit_length() - 1) == row
    key_pos = jnp.bitwise_and(col, seq - 1).astype(F32)
    scale = head ** -0.5

    def e_copy(half, j, core):
        return rcopy(xc.at[j, half, core], xc.at[j, half, core], e_send.at[half, j], e_recv.at[half, j], pair)

    def out_copy(half, j):
        dst = out.at[pl.ds(half * hr, hr), pl.ds(al(j * TN, TN), TN)]
        return pltpu.make_async_copy(xc.at[j, half, c], dst, e_send.at[half, j])

    def y_copy(half, j):
        return rcopy(yp.at[j, c, half, 1], yr.at[half, j], y_send.at[half, j], y_recv.at[half, j], ypeer)

    def d_copy(j):
        return rcopy(yp.at[j, oc], dr.at[j], d_send.at[j], d_recv.at[j], pair)

    def finish(half, after):
        def one(j, carry):
            y_copy(half, j).wait_recv()
            y = (yp[j, c, half, 0] + dr[j, half, 0] + yr[half, j]).astype(BF16).astype(F32)
            xc[j, half, c] = (x1[0, j, half, c].astype(F32) + y).astype(BF16)
            after(j)
            return carry

        lax.fori_loop(0, nch, one, 0)

    def exchange(half):
        finish(half, lambda j: e_copy(half, j, c).start())
        for j in range(nch):
            e_copy(half, j, oc).wait_recv()
            e_copy(half, j, c).wait_send()

    def sums_sent():
        for j in range(nch):
            d_copy(j).wait_send()
            for half in range(2):
                y_copy(half, j).wait_send()

    def xy_copy(half, j):
        mine = c * nq + j
        return rcopy(x1.at[0, mine, half], x1.at[1, mine, half], xy_send.at[half, j], xy_recv.at[half, j], ypeer)

    def xp_copy(half, j, core):
        at = x1.at[0, core * nq + j, half]
        return rcopy(at, at, xp_send.at[half, j], xp_recv.at[half, j], pair)

    def xf_copy(half, j, core):
        at = x1.at[1, core * nq + j, half]
        return rcopy(at, at, xf_send.at[half, j], xf_recv.at[half, j], pair)

    def o_copy(half, core, cc):
        at = oa.at[cc, half, pl.ds(al(core * hr, hr), hr)]
        return rcopy(at, at, o_send.at[half, core], o_recv.at[half, core], pair)

    def attention_half(layer, half):
        first = half == 0

        def arrive(rs):
            @pl.when(first)
            def _():
                for r in rs:
                    wait_top(slot_of(layer, r))

        def refill(rs):
            @pl.when(jnp.logical_not(first))
            def _():
                for r in rs:
                    fill_gu(layer, r)

        with jax.named_scope("norm_a"):
            norm_half(lambda j, k: xc[j, half, k], ag_ref, layer, 0)

        def both_cores(table):
            return jnp.concatenate([table[pl.ds(al((k * 2 + half) * hr, hr), hr), :] for k in range(2)], axis=0)

        cos_v = both_cores(cos_t)
        sin_v = both_cores(sin_t)

        def rope(v):
            return (v * cos_v + pltpu.roll(v, head // 2, 1) * sin_v).astype(BF16).astype(F32)

        def qkv(r):
            y = dot(h[:2 * hr, :], ring[slot_of(layer, r), :d_model, :])
            for k in range(2):
                part = y[:, k * head:(k + 1) * head]
                if r < nq:
                    qf[r * 2 + k] = rope(part)
                elif r == nq:
                    kn[k] = rope(part)
                else:
                    vn[k] = part.astype(BF16).astype(F32)

        with jax.named_scope("qkv"):
            for rs in spans(QKV_STEPS, r_o):
                arrive(rs)
                for r in rs:
                    qkv(r)
                refill(rs)

        def core_body(core, carry):
            for cp in cache_copies(layer, half, core):
                cp.wait()
            @pl.when(core >= 0)
            def _():
                for gi in range(hr // GS):
                    n_old = len_t[pl.ds(al((core * 2 + half) * hr + gi * GS, GS), GS), :head]
                    n_old = jnp.concatenate([n_old] * (GS * seq // head), axis=1)
                    valid = own_keys & (key_pos < n_old)
                    r0 = al(core * hr + gi * GS, GS)
                    for k in range(2):
                        q = qf[k * group:(k + 1) * group, pl.ds(r0, GS), :]
                        keys = kb[core, gi * GS:(gi + 1) * GS, k].reshape(GS * seq, head)
                        sc = lax.dot_general(q.reshape(group * GS, head).astype(BF16), keys, (((1,), (1,)), ((), ())),
                                             preferred_element_type=F32)
                        sc = sc.reshape(group, GS, GS * seq) * scale
                        sc = jnp.where(valid[None], sc, -1e30)
                        k_new = kn[k, pl.ds(r0, GS), :]
                        self_sc = jnp.sum(q * k_new[None], axis=-1, keepdims=True) * scale
                        top = jnp.maximum(jnp.max(sc, axis=-1, keepdims=True), self_sc)
                        e = jnp.exp(sc - top)
                        self_e = jnp.exp(self_sc - top)
                        total = jnp.sum(e, axis=-1, keepdims=True) + self_e
                        p_s[gi, k] = e.reshape(group * GS, GS * seq).astype(BF16)
                        tot_s[gi, k] = jnp.broadcast_to(total, (group, GS, head))
                        self_s[gi, k] = jnp.broadcast_to(self_e, (group, GS, head))

            @pl.when(core >= 0)
            def _():
                for gi in range(hr // GS):
                    r0 = al(core * hr + gi * GS, GS)
                    for k in range(2):
                        vals = vb[core, gi * GS:(gi + 1) * GS, k].reshape(GS * seq, head)
                        mix = dot(p_s[gi, k], vals).reshape(group, GS, head)
                        mix = mix + self_s[gi, k].astype(BF16).astype(F32) * vn[k, pl.ds(r0, GS), :][None]
                        of[k * group:(k + 1) * group, gi * GS:(gi + 1) * GS, :] = mix / tot_s[gi, k]

            for hh in range(heads // 2):
                oa[c, half, pl.ds(al(core * hr, hr), hr), hh * head:(hh + 1) * head] = of[hh].astype(BF16)
            o_copy(half, core, c).start()

            @pl.when(first)
            def _():
                for cp in cache_copies(layer, 1, core):
                    cp.start()

            @pl.when(jnp.logical_not(first) & (layer + 1 < n_layers))
            def _():
                for cp in cache_copies(layer + 1, 0, core):
                    cp.start()

            return carry

        with jax.named_scope("attn"):
            lax.fori_loop(0, 2, core_body, 0)

        with jax.named_scope("w_o_own"):
            arrive(range(r_o, r_gu))
            for i in range(nq):
                w = ring[slot_of(layer, r_o + i), pl.ds(al(c * half_d, half_d), half_d), :]
                acc_s[i] = dot(oa[c, half], w) + xc[c * nq + i, half].reshape(2 * hr, TN).astype(F32)
        with jax.named_scope("o_wait"):
            @pl.when(jnp.logical_not(first))
            def _():
                for j in range(nq):
                    xy_copy(0, j).wait_recv()
                    xf_copy(0, j, c).start()

            for core in range(2):
                o_copy(half, core, oc).wait_recv()
        with jax.named_scope("w_o"):
            for js in spans(O_STEPS, nq):
                for i in js:
                    w = ring[slot_of(layer, r_o + i), pl.ds(al(oc * half_d, half_d), half_d), :]
                    acc = acc_s[i] + dot(oa[oc, half], w)
                    x1[0, c * nq + i, half] = acc.astype(BF16).reshape(2, hr, TN)
                for i in js:
                    xy_copy(half, i).start()
                    xp_copy(half, i, c).start()
                refill([r_o + i for i in js])

    def layer_body(layer, carry):
        not_last = layer + 1 < n_layers

        def half_body(half, carry):
            @pl.when((half == 1) & (layer == 0))
            def _():
                for jhk in rows_in[1]:
                    row_copy(*jhk).wait()

            @pl.when((half == 1) & (layer > 0))
            def _():
                with jax.named_scope("finish_b"):
                    exchange(1)
                    sums_sent()

            attention_half(layer, half)
            return carry

        lax.fori_loop(0, 2, half_body, 0)

        with jax.named_scope("ag_wait"):
            for half in range(2):
                for j in range(nq):
                    xp_copy(half, j, oc).wait_recv()
                norm_half(lambda j, k: x1[0, j, half, k], fg_ref, layer, half * 2 * hr)
                if half:
                    for j in range(nq):
                        xy_copy(half, j).wait_recv()
                        xf_copy(half, j, c).start()
                for j in range(nq):
                    xf_copy(half, j, oc).wait_recv()
                norm_half(lambda j, k: x1[1, j, half, k], fg_ref, layer, (2 + half) * 2 * hr)

        def gate_up(first, count, fill):
            slots = [slot_of(layer, r_gu + first + i) for i in range(count)]
            for slot in slots:
                wait_top(slot)
            for i, slot in enumerate(slots):
                y = dot(h[...], ring[slot, :d_model, :])
                gate = y[:, :128]
                act = gate * (1.0 / (1.0 + jnp.exp(-gate))) * y[:, 128:]
                u[:, pl.ds(al((first + i) * 128, 128), 128)] = act.astype(BF16)
            for i in range(count):
                fill(first + i)

        n_a = ngu - NS
        n_b = nch

        def gu_a(i, carry):
            gate_up(i * GU, GU, lambda t: fill_gu(layer, t + NS))
            return carry

        def gu_b(i, carry):
            gate_up(n_a + i * GU, GU, lambda t: fill_dn(layer, t - n_a))
            return carry

        def fill_next(t):
            @pl.when(not_last)
            def _():
                fill_attn(layer + 1, t - n_a - n_b)

        assert n_a % GU == 0 and n_b % GU == 0
        with jax.named_scope("gate_up"):
            lax.fori_loop(0, n_a // GU, gu_a, 0)
            lax.fori_loop(0, n_b // GU, gu_b, 0)
            gate_up(n_a + n_b, ngu - n_a - n_b, fill_next)

        for half in range(2):
            for j in range(nq):
                xf_copy(half, j, c).wait_send()
                xy_copy(half, j).wait_send()
                xp_copy(half, j, c).wait_send()
            for core in range(2):
                o_copy(half, core, c).wait_send()

        def pair_sum(j):
            d_copy(j).wait_recv()
            for half in range(2):
                yp[j, c, half, 1] = yp[j, c, half, 1] + dr[j, half, 1]
            y_copy(0, j).start()

        def down(js, before):
            slots = [slot_of(layer, r_dn + j) for j in js]
            for slot in slots:
                wait_full(slot)
            for j, slot in zip(js, slots):
                y = dot(u[...], ring[slot])
                for chip in range(2):
                    for half in range(2):
                        for core in range(2):
                            r0 = ((chip * 2 + half) * 2 + core) * hr
                            yp[j, core, half, chip] = y[r0:r0 + hr, :]
            for j in js:
                d_copy(j).start()

            @pl.when(not_last)
            def _():
                for j in js:
                    fill_attn(layer + 1, j + ngu - n_a - n_b)

            for j in before:
                pair_sum(j)

        with jax.named_scope("down"):
            steps = spans(DN_STEPS, nch)
            for js, before in zip(steps, [[]] + steps[:-1]):
                down(js, before)
        with jax.named_scope("pair_last"):
            for j in steps[-1]:
                pair_sum(j)
            for j in range(nch):
                y_copy(1, j).start()

        with jax.named_scope("finish_a"):
            @pl.when(not_last)
            def _():
                exchange(0)

            @pl.when(jnp.logical_not(not_last))
            def _():
                finish(0, lambda j: out_copy(0, j).start())

        return carry

    lax.fori_loop(0, n_layers, layer_body, 0)
    with jax.named_scope("finish_b"):
        finish(1, lambda j: out_copy(1, j).start())
        sums_sent()
        for half in range(2):
            for j in range(nch):
                out_copy(half, j).wait()


def solution(mesh):
    batch_axes = ('inst', 'dev')
    in_specs = (
        P(batch_axes, None),
        P(batch_axes),
        P(None, batch_axes, None, None, None),
        P(None, batch_axes, None, None, None),
        P(), P(), P(), P(), P(),
        P(None, None, 'dev'),
        P(None, None, 'dev'),
        P(None, 'dev', None),
    )
    out_specs = P(('inst', 'dev', 'side'), None)
    n_side = mesh.shape['side']

    def device_fn(hidden, cache_len, k_cache, v_cache, w_q, w_kv, w_o, attn_gain, ffn_gain, w_gate, w_up, w_down):
        n_layers, d_model, _ = w_q.shape
        kv_heads, seq, head = k_cache.shape[2:]
        heads = w_q.shape[2] // head
        rows = hidden.shape[0] // n_side
        ff = w_gate.shape[2] // 2
        nch = d_model // TN
        nq = nch // 2
        hr = rows // 2
        group = heads // kv_heads
        half_dim = head // 2
        freqs = np.float32(ROPE_BASE) ** (-np.arange(half_dim, dtype=np.float32) / np.float32(half_dim))
        freqs = jnp.asarray(np.concatenate([freqs, freqs])[None].astype(np.float32))
        lengths = cache_len.reshape(n_side // 2, 2 * rows)
        dims = (n_layers, d_model, ff, heads, kv_heads, head, seq)
        vmem = pl.BlockSpec(memory_space=pltpu.VMEM)
        hbm = pl.BlockSpec(memory_space=pl.ANY)
        dma = pltpu.SemaphoreType.DMA
        return pl.pallas_call(
            functools.partial(kernel, dims),
            name='decode_layers',
            out_shape=jax.ShapeDtypeStruct((rows, d_model), BF16),
            in_specs=[vmem] * 4 + [hbm] * 9,
            out_specs=hbm,
            scratch_shapes=[
                pltpu.VMEM((NS, ff, TN), BF16),
                pltpu.VMEM((nch, 2, 2, hr, TN), BF16),
                pltpu.VMEM((2, nch, 2, 2, hr, TN), BF16),
                pltpu.VMEM((4 * rows, d_model), BF16),
                pltpu.VMEM((heads // 2, rows, head), F32),
                pltpu.VMEM((2, rows, head), F32),
                pltpu.VMEM((2, rows, head), F32),
                pltpu.VMEM((hr // GS, 2, group * GS, GS * seq), BF16),
                pltpu.VMEM((hr // GS, 2, group, GS, head), F32),
                pltpu.VMEM((hr // GS, 2, group, GS, head), F32),
                pltpu.VMEM((heads // 2, hr, head), F32),
                pltpu.VMEM((2, 2, rows, d_model // 2), BF16),
                pltpu.VMEM((nq, rows, TN), F32),
                pltpu.VMEM((4 * rows, ff), BF16),
                pltpu.VMEM((nch, 2, 2, 2, hr, TN), F32),
                pltpu.VMEM((nch, 2, 2, hr, TN), F32),
                pltpu.VMEM((2, nch, hr, TN), F32),
                pltpu.VMEM((2, hr, 2, seq, head), BF16),
                pltpu.VMEM((2, hr, 2, seq, head), BF16),
                pltpu.VMEM((2 * rows, head), F32),
                pltpu.VMEM((2 * rows, head), F32),
                pltpu.VMEM((2 * rows, 2 * rows), F32),
                dma((NS,)), dma((2, 2)), dma((nch, 2, 2)),
                dma((2, 2)), dma((2, 2)),
                dma((2, nq)), dma((2, nq)), dma((2, nq)), dma((2, nq)), dma((2, nq)), dma((2, nq)),
                dma((nch,)), dma((nch,)), dma((2, nch)), dma((2, nch)), dma((2, nch)), dma((2, nch)),
            ],
            compiler_params=pltpu.CompilerParams(
                collective_id=0, has_side_effects=True, vmem_limit_bytes=67043328),
        )(lengths, freqs, attn_gain, ffn_gain, hidden, k_cache, v_cache, w_q, w_kv, w_o, w_gate, w_up, w_down)

    return jax.shard_map(device_fn, mesh=mesh, in_specs=in_specs, out_specs=out_specs, check_vma=False)
```

```python
import functools

import jax
import jax.numpy as jnp
import numpy as np
from jax import lax
from jax.experimental import pallas as pl
from jax.experimental.pallas import tpu as pltpu
from jax.sharding import PartitionSpec as P

EPS = 1e-5
ROPE_BASE = 10000.0
MESH = pl.DeviceIdType.MESH
F32 = jnp.float32
BF16 = jnp.bfloat16

TN = 256
NS = 16
GS = 8
GU = 7
GU_EARLY = 2
LATE_STEPS = (3, 4, 3, 4)
DN_STEPS = (2, 2, 2, 2, 2, 2, 2)
QKV_STEPS = (4, 5)
O_STEPS = (2, 2, 3)


def spans(steps, total):
    assert sum(steps) == total
    out, at = [], 0
    for n in steps:
        out.append(list(range(at, at + n)))
        at += n
    return out


def dot(lhs, rhs):
    return jnp.dot(lhs, rhs, preferred_element_type=F32)


def kernel(dims, len_ref, freq_ref, ag_ref, fg_ref, hid, kc, vc, wq, wkv, wo, wg, wu, wd, out,
           ring, xc, x1, h, qf, kn, vn, p_s, tot_s, self_s, of, oa, acc_s, u, yp, dr, yr, kb, vb, cos_t, sin_t, len_t,
           ring_sem, cache_sem, in_sem, o_send, o_recv, xp_send, xp_recv, xy_send, xy_recv, xf_send, xf_recv,
           d_send, d_recv, y_send, y_recv, e_send, e_recv):
    n_layers, d_model, ff, heads, kv_heads, head, seq = dims
    half_d = d_model // 2
    nch = d_model // TN
    nq = half_d // TN
    hr = xc.shape[3]
    ngu = ff // 128
    group = heads // kv_heads
    r_o = nq + 2
    r_gu = r_o + nq
    r_dn = r_gu + ngu
    tiles = r_dn + nch
    assert r_gu == NS

    side = lax.axis_index("side")
    dev = lax.axis_index("dev")
    c = lax.rem(side, 2)
    oc = 1 - c
    base = (side - c) * (2 * hr)
    pair = {"side": side + 1 - 2 * c}
    ypeer = {"dev": 1 - dev}

    barrier = pltpu.get_barrier_semaphore()
    pl.semaphore_signal(barrier, inc=1, device_id=pair, device_id_type=MESH)
    pl.semaphore_signal(barrier, inc=1, device_id=ypeer, device_id_type=MESH)

    def rcopy(src, dst, ssem, rsem, where):
        return pltpu.make_async_remote_copy(
            src_ref=src, dst_ref=dst, send_sem=ssem, recv_sem=rsem, device_id=where, device_id_type=MESH)

    def al(v, m):
        return pl.multiple_of(v, m)

    def slot_of(layer, r):
        return lax.rem(layer * tiles + r, NS)

    def fill_attn(layer, r):
        slot = slot_of(layer, r)
        top = ring.at[slot, pl.ds(0, d_model)]
        if r < nq:
            src = wq.at[layer, :, pl.ds(al(c * half_d + r * TN, TN), TN)]
        elif r < r_o:
            src = wkv.at[layer, :, pl.ds(al((r - nq) * (2 * TN) + c * TN, TN), TN)]
        else:
            src = wo.at[layer, :, pl.ds(al(c * half_d + (r - r_o) * TN, TN), TN)]
        pltpu.make_async_copy(src, top, ring_sem.at[slot]).start()

    def fill_gu(layer, i):
        slot = slot_of(layer, r_gu + i)
        col = al(c * ff + i * 128, 128)
        for k, w in enumerate((wg, wu)):
            pltpu.make_async_copy(
                w.at[layer, :, pl.ds(col, 128)], ring.at[slot, pl.ds(0, d_model), pl.ds(k * 128, 128)],
                ring_sem.at[slot]).start()

    def fill_dn(layer, j):
        slot = slot_of(layer, r_dn + j)
        pltpu.make_async_copy(
            wd.at[layer, pl.ds(al(c * ff, 128), ff), pl.ds(al(j * TN, TN), TN)], ring.at[slot], ring_sem.at[slot]).start()

    def wait_top(slot):
        pltpu.make_async_copy(wq.at[0, :, pl.ds(0, TN)], ring.at[slot, pl.ds(0, d_model)], ring_sem.at[slot]).wait()

    def wait_full(slot):
        pltpu.make_async_copy(wd.at[0, pl.ds(0, ff), pl.ds(0, TN)], ring.at[slot], ring_sem.at[slot]).wait()

    def cache_copies(layer, half, core):
        src = pl.ds(al(base + core * (2 * hr) + half * hr, hr), hr)
        hd = pl.ds(c * 2, 2)
        return (pltpu.make_async_copy(kc.at[layer, src, hd], kb.at[core], cache_sem.at[core, 0]),
                pltpu.make_async_copy(vc.at[layer, src, hd], vb.at[core], cache_sem.at[core, 1]))

    def norm_half(read, gain, layer, dst_row):
        for k in range(2):
            total = jnp.zeros((hr, TN), F32)
            for j in range(nch):
                v = read(j, k).astype(F32)
                total = total + v * v
            inv = lax.rsqrt(jnp.sum(total, axis=-1, keepdims=True) * (1.0 / d_model) + EPS)
            r0 = dst_row + k * hr
            for j in range(nch):
                v = read(j, k).astype(F32)
                g = gain[pl.ds(layer, 1), j * TN:(j + 1) * TN]
                h[r0:r0 + hr, j * TN:(j + 1) * TN] = (v * inv * g).astype(BF16)

    def row_copy(j, half, k):
        src = hid.at[pl.ds(al(base + (k * 2 + half) * hr, hr), hr), pl.ds(j * TN, TN)]
        return pltpu.make_async_copy(src, xc.at[j, half, k], in_sem.at[j, half, k])

    rows_in = [[(j, half, k) for j in range(nch) for k in range(2)] for half in range(2)]
    for jhk in rows_in[0]:
        row_copy(*jhk).start()
    for r in range(4):
        fill_attn(0, r)

    n_pos = 4 * hr
    lens = len_ref[pl.ds(lax.div(side, 2), 1), :].astype(F32)
    len_t[...] = jnp.broadcast_to(lens, (n_pos, n_pos)).T
    angle = len_t[:, :head] * freq_ref[...]
    lane = lax.broadcasted_iota(jnp.int32, (n_pos, head), 1)
    cos_t[...] = jnp.cos(angle)
    sin_t[...] = jnp.sin(angle) * jnp.where(lane < head // 2, -1.0, 1.0)

    for jhk in rows_in[0]:
        row_copy(*jhk).wait()
    for r in range(4, r_o):
        fill_attn(0, r)
    for core in range(2):
        for cp in cache_copies(0, 0, core):
            cp.start()
    for jhk in rows_in[1]:
        row_copy(*jhk).start()
    for r in range(r_o, r_gu):
        fill_attn(0, r)
    pl.semaphore_wait(barrier, 2)

    col = lax.broadcasted_iota(jnp.int32, (GS, GS * seq), 1)
    row = lax.broadcasted_iota(jnp.int32, (GS, GS * seq), 0)
    own_keys = lax.shift_right_logical(col, seq.bit_length() - 1) == row
    key_pos = jnp.bitwise_and(col, seq - 1).astype(F32)
    scale = head ** -0.5

    def e_copy(half, j, core):
        return rcopy(xc.at[j, half, core], xc.at[j, half, core], e_send.at[half, j], e_recv.at[half, j], pair)

    def out_copy(half, j):
        dst = out.at[pl.ds(half * hr, hr), pl.ds(al(j * TN, TN), TN)]
        return pltpu.make_async_copy(xc.at[j, half, c], dst, e_send.at[half, j])

    def y_copy(half, j):
        return rcopy(yp.at[j, c, half, 1], yr.at[half, j], y_send.at[half, j], y_recv.at[half, j], ypeer)

    def d_copy(j):
        return rcopy(yp.at[j, oc], dr.at[j], d_send.at[j], d_recv.at[j], pair)

    def finish(half, after):
        def one(j, carry):
            y_copy(half, j).wait_recv()
            y = (yp[j, c, half, 0] + dr[j, half, 0] + yr[half, j]).astype(BF16).astype(F32)
            xc[j, half, c] = (x1[0, j, half, c].astype(F32) + y).astype(BF16)
            after(j)
            return carry

        lax.fori_loop(0, nch, one, 0)

    def exchange(half):
        finish(half, lambda j: e_copy(half, j, c).start())
        for j in range(nch):
            e_copy(half, j, oc).wait_recv()
            e_copy(half, j, c).wait_send()

    def sums_sent():
        for j in range(nch):
            d_copy(j).wait_send()
            for half in range(2):
                y_copy(half, j).wait_send()

    def xy_copy(half, j):
        mine = c * nq + j
        return rcopy(x1.at[0, mine, half], x1.at[1, mine, half], xy_send.at[half, j], xy_recv.at[half, j], ypeer)

    def xp_copy(half, j, core):
        at = x1.at[0, core * nq + j, half]
        return rcopy(at, at, xp_send.at[half, j], xp_recv.at[half, j], pair)

    def xf_copy(half, j, core):
        at = x1.at[1, core * nq + j, half]
        return rcopy(at, at, xf_send.at[half, j], xf_recv.at[half, j], pair)

    def o_copy(half, core, cc):
        at = oa.at[cc, half, pl.ds(al(core * hr, hr), hr)]
        return rcopy(at, at, o_send.at[half, core], o_recv.at[half, core], pair)

    def attention_half(layer, half):
        first = half == 0

        def arrive(rs):
            @pl.when(first)
            def _():
                for r in rs:
                    wait_top(slot_of(layer, r))

        def refill(rs):
            @pl.when(jnp.logical_not(first))
            def _():
                for r in rs:
                    fill_gu(layer, r)

        with jax.named_scope("norm_a"):
            norm_half(lambda j, k: xc[j, half, k], ag_ref, layer, 0)

        def both_cores(table):
            return jnp.concatenate([table[pl.ds(al((k * 2 + half) * hr, hr), hr), :] for k in range(2)], axis=0)

        cos_v = both_cores(cos_t)
        sin_v = both_cores(sin_t)

        def rope(v):
            return (v * cos_v + pltpu.roll(v, head // 2, 1) * sin_v).astype(BF16).astype(F32)

        def qkv(r):
            y = dot(h[:2 * hr, :], ring[slot_of(layer, r), :d_model, :])
            for k in range(2):
                part = y[:, k * head:(k + 1) * head]
                if r < nq:
                    qf[r * 2 + k] = rope(part)
                elif r == nq:
                    kn[k] = rope(part)
                else:
                    vn[k] = part.astype(BF16).astype(F32)

        with jax.named_scope("qkv"):
            for rs in spans(QKV_STEPS, r_o):
                arrive(rs)
                for r in rs:
                    qkv(r)
                refill(rs)

        def core_body(core, carry):
            for cp in cache_copies(layer, half, core):
                cp.wait()
            @pl.when(core >= 0)
            def _():
                for gi in range(hr // GS):
                    n_old = len_t[pl.ds(al((core * 2 + half) * hr + gi * GS, GS), GS), :head]
                    n_old = jnp.concatenate([n_old] * (GS * seq // head), axis=1)
                    valid = own_keys & (key_pos < n_old)
                    r0 = al(core * hr + gi * GS, GS)
                    for k in range(2):
                        q = qf[k * group:(k + 1) * group, pl.ds(r0, GS), :]
                        keys = kb[core, gi * GS:(gi + 1) * GS, k].reshape(GS * seq, head)
                        sc = lax.dot_general(q.reshape(group * GS, head).astype(BF16), keys, (((1,), (1,)), ((), ())),
                                             preferred_element_type=F32)
                        sc = sc.reshape(group, GS, GS * seq) * scale
                        sc = jnp.where(valid[None], sc, -1e30)
                        k_new = kn[k, pl.ds(r0, GS), :]
                        self_sc = jnp.sum(q * k_new[None], axis=-1, keepdims=True) * scale
                        top = jnp.maximum(jnp.max(sc, axis=-1, keepdims=True), self_sc)
                        e = jnp.exp(sc - top)
                        self_e = jnp.exp(self_sc - top)
                        total = jnp.sum(e, axis=-1, keepdims=True) + self_e
                        p_s[gi, k] = e.reshape(group * GS, GS * seq).astype(BF16)
                        tot_s[gi, k] = jnp.broadcast_to(total, (group, GS, head))
                        self_s[gi, k] = jnp.broadcast_to(self_e, (group, GS, head))

            @pl.when(core >= 0)
            def _():
                for gi in range(hr // GS):
                    r0 = al(core * hr + gi * GS, GS)
                    for k in range(2):
                        vals = vb[core, gi * GS:(gi + 1) * GS, k].reshape(GS * seq, head)
                        mix = dot(p_s[gi, k], vals).reshape(group, GS, head)
                        mix = mix + self_s[gi, k].astype(BF16).astype(F32) * vn[k, pl.ds(r0, GS), :][None]
                        of[k * group:(k + 1) * group, gi * GS:(gi + 1) * GS, :] = mix / tot_s[gi, k]

            for hh in range(heads // 2):
                oa[c, half, pl.ds(al(core * hr, hr), hr), hh * head:(hh + 1) * head] = of[hh].astype(BF16)
            o_copy(half, core, c).start()

            @pl.when(first)
            def _():
                for cp in cache_copies(layer, 1, core):
                    cp.start()

            @pl.when(jnp.logical_not(first) & (layer + 1 < n_layers))
            def _():
                for cp in cache_copies(layer + 1, 0, core):
                    cp.start()

            return carry

        with jax.named_scope("attn"):
            lax.fori_loop(0, 2, core_body, 0)

        with jax.named_scope("w_o_own"):
            arrive(range(r_o, r_gu))
            for i in range(nq):
                w = ring[slot_of(layer, r_o + i), pl.ds(al(c * half_d, half_d), half_d), :]
                acc_s[i] = dot(oa[c, half], w) + xc[c * nq + i, half].reshape(2 * hr, TN).astype(F32)
        with jax.named_scope("o_wait"):
            @pl.when(jnp.logical_not(first))
            def _():
                for j in range(nq):
                    xy_copy(0, j).wait_recv()
                    xf_copy(0, j, c).start()

            for core in range(2):
                o_copy(half, core, oc).wait_recv()
        with jax.named_scope("w_o"):
            for js in spans(O_STEPS, nq):
                for i in js:
                    w = ring[slot_of(layer, r_o + i), pl.ds(al(oc * half_d, half_d), half_d), :]
                    acc = acc_s[i] + dot(oa[oc, half], w)
                    x1[0, c * nq + i, half] = acc.astype(BF16).reshape(2, hr, TN)
                for i in js:
                    xy_copy(half, i).start()
                    xp_copy(half, i, c).start()
                refill([r_o + i for i in js])

    def layer_body(layer, carry):
        not_last = layer + 1 < n_layers

        def half_body(half, carry):
            @pl.when((half == 1) & (layer == 0))
            def _():
                for jhk in rows_in[1]:
                    row_copy(*jhk).wait()

            @pl.when((half == 1) & (layer > 0))
            def _():
                with jax.named_scope("finish_b"):
                    exchange(1)
                    sums_sent()

            attention_half(layer, half)
            return carry

        lax.fori_loop(0, 2, half_body, 0)

        def norm_f(chip, half):
            read = lambda j, k: x1[chip, j, half, k]
            norm_half(read, fg_ref, layer, (chip * 2 + half) * 2 * hr)

        with jax.named_scope("ag_first"):
            for j in range(nq):
                xp_copy(0, j, oc).wait_recv()
            norm_f(0, 0)
            for j in range(nq):
                xf_copy(0, j, oc).wait_recv()
            norm_f(1, 0)
            for j in range(nq):
                xp_copy(1, j, oc).wait_recv()
            norm_f(0, 1)

        def gate_up(first, count, r0, r1, wait, fill):
            slots = [slot_of(layer, r_gu + first + i) for i in range(count)]
            if wait:
                for slot in slots:
                    wait_top(slot)
            for i, slot in enumerate(slots):
                y = dot(h[r0:r1, :], ring[slot, :d_model, :])
                gate = y[:, :128]
                act = gate * (1.0 / (1.0 + jnp.exp(-gate))) * y[:, 128:]
                u[r0:r1, pl.ds(al((first + i) * 128, 128), 128)] = act.astype(BF16)
            if fill:
                for i in range(count):
                    fill(first + i)

        n_a = ngu - NS
        n_b = nch
        n_rows = 8 * hr
        late = 6 * hr
        assert n_b % GU == 0 and GU_EARLY * GU < NS < n_a

        def gu_early(i, carry):
            gate_up(i * GU, GU, 0, late, True, None)

            def forward(j, carry):
                xy_copy(1, j).wait_recv()
                xf_copy(1, j, c).start()
                return carry

            lax.fori_loop(nq * i // GU_EARLY, nq * (i + 1) // GU_EARLY, forward, 0)
            return carry

        def fill_a(t):
            fill_gu(layer, t + NS)

        def gu_b(i, carry):
            gate_up(n_a + i * GU, GU, 0, n_rows, True, lambda t: fill_dn(layer, t - n_a))
            return carry

        def fill_next(t):
            @pl.when(not_last)
            def _():
                fill_attn(layer + 1, t - n_a - n_b)

        with jax.named_scope("gu_early"):
            lax.fori_loop(0, GU_EARLY, gu_early, 0)
        with jax.named_scope("ag_last"):
            for j in range(nq):
                xf_copy(1, j, oc).wait_recv()
            norm_f(1, 1)
        with jax.named_scope("gu_late"):
            for ts in spans(LATE_STEPS, GU_EARLY * GU):
                gate_up(ts[0], len(ts), late, n_rows, False, fill_a)
        with jax.named_scope("gate_up"):
            gate_up(GU_EARLY * GU, NS - GU_EARLY * GU, 0, n_rows, True, fill_a)
            gate_up(NS, n_a - NS, 0, n_rows, True, fill_a)
            lax.fori_loop(0, n_b // GU, gu_b, 0)
            gate_up(n_a + n_b, ngu - n_a - n_b, 0, n_rows, True, fill_next)

        for half in range(2):
            for j in range(nq):
                xf_copy(half, j, c).wait_send()
                xy_copy(half, j).wait_send()
                xp_copy(half, j, c).wait_send()
            for core in range(2):
                o_copy(half, core, c).wait_send()

        def pair_sum(j):
            d_copy(j).wait_recv()
            for half in range(2):
                yp[j, c, half, 1] = yp[j, c, half, 1] + dr[j, half, 1]
            y_copy(0, j).start()

        def down(js, before):
            slots = [slot_of(layer, r_dn + j) for j in js]
            for slot in slots:
                wait_full(slot)
            for j, slot in zip(js, slots):
                y = dot(u[...], ring[slot])
                for chip in range(2):
                    for half in range(2):
                        for core in range(2):
                            r0 = ((chip * 2 + half) * 2 + core) * hr
                            yp[j, core, half, chip] = y[r0:r0 + hr, :]
            for j in js:
                d_copy(j).start()

            @pl.when(not_last)
            def _():
                for j in js:
                    fill_attn(layer + 1, j + ngu - n_a - n_b)

            for j in before:
                pair_sum(j)

        with jax.named_scope("down"):
            steps = spans(DN_STEPS, nch)
            for js, before in zip(steps, [[]] + steps[:-1]):
                down(js, before)
        with jax.named_scope("pair_last"):
            for j in steps[-1]:
                pair_sum(j)
            for j in range(nch):
                y_copy(1, j).start()

        with jax.named_scope("finish_a"):
            @pl.when(not_last)
            def _():
                exchange(0)

            @pl.when(jnp.logical_not(not_last))
            def _():
                finish(0, lambda j: out_copy(0, j).start())

        return carry

    lax.fori_loop(0, n_layers, layer_body, 0)
    with jax.named_scope("finish_b"):
        finish(1, lambda j: out_copy(1, j).start())
        sums_sent()
        for half in range(2):
            for j in range(nch):
                out_copy(half, j).wait()


def solution(mesh):
    batch_axes = ('inst', 'dev')
    in_specs = (
        P(batch_axes, None),
        P(batch_axes),
        P(None, batch_axes, None, None, None),
        P(None, batch_axes, None, None, None),
        P(), P(), P(), P(), P(),
        P(None, None, 'dev'),
        P(None, None, 'dev'),
        P(None, 'dev', None),
    )
    out_specs = P(('inst', 'dev', 'side'), None)
    n_side = mesh.shape['side']

    def device_fn(hidden, cache_len, k_cache, v_cache, w_q, w_kv, w_o, attn_gain, ffn_gain, w_gate, w_up, w_down):
        n_layers, d_model, _ = w_q.shape
        kv_heads, seq, head = k_cache.shape[2:]
        heads = w_q.shape[2] // head
        rows = hidden.shape[0] // n_side
        ff = w_gate.shape[2] // 2
        nch = d_model // TN
        nq = nch // 2
        hr = rows // 2
        group = heads // kv_heads
        half_dim = head // 2
        freqs = np.float32(ROPE_BASE) ** (-np.arange(half_dim, dtype=np.float32) / np.float32(half_dim))
        freqs = jnp.asarray(np.concatenate([freqs, freqs])[None].astype(np.float32))
        lengths = cache_len.reshape(n_side // 2, 2 * rows)
        dims = (n_layers, d_model, ff, heads, kv_heads, head, seq)
        vmem = pl.BlockSpec(memory_space=pltpu.VMEM)
        hbm = pl.BlockSpec(memory_space=pl.ANY)
        dma = pltpu.SemaphoreType.DMA
        return pl.pallas_call(
            functools.partial(kernel, dims),
            name='decode_layers',
            out_shape=jax.ShapeDtypeStruct((rows, d_model), BF16),
            in_specs=[vmem] * 4 + [hbm] * 9,
            out_specs=hbm,
            scratch_shapes=[
                pltpu.VMEM((NS, ff, TN), BF16),
                pltpu.VMEM((nch, 2, 2, hr, TN), BF16),
                pltpu.VMEM((2, nch, 2, 2, hr, TN), BF16),
                pltpu.VMEM((4 * rows, d_model), BF16),
                pltpu.VMEM((heads // 2, rows, head), F32),
                pltpu.VMEM((2, rows, head), F32),
                pltpu.VMEM((2, rows, head), F32),
                pltpu.VMEM((hr // GS, 2, group * GS, GS * seq), BF16),
                pltpu.VMEM((hr // GS, 2, group, GS, head), F32),
                pltpu.VMEM((hr // GS, 2, group, GS, head), F32),
                pltpu.VMEM((heads // 2, hr, head), F32),
                pltpu.VMEM((2, 2, rows, d_model // 2), BF16),
                pltpu.VMEM((nq, rows, TN), F32),
                pltpu.VMEM((4 * rows, ff), BF16),
                pltpu.VMEM((nch, 2, 2, 2, hr, TN), F32),
                pltpu.VMEM((nch, 2, 2, hr, TN), F32),
                pltpu.VMEM((2, nch, hr, TN), F32),
                pltpu.VMEM((2, hr, 2, seq, head), BF16),
                pltpu.VMEM((2, hr, 2, seq, head), BF16),
                pltpu.VMEM((2 * rows, head), F32),
                pltpu.VMEM((2 * rows, head), F32),
                pltpu.VMEM((2 * rows, 2 * rows), F32),
                dma((NS,)), dma((2, 2)), dma((nch, 2, 2)),
                dma((2, 2)), dma((2, 2)),
                dma((2, nq)), dma((2, nq)), dma((2, nq)), dma((2, nq)), dma((2, nq)), dma((2, nq)),
                dma((nch,)), dma((nch,)), dma((2, nch)), dma((2, nch)), dma((2, nch)), dma((2, nch)),
            ],
            compiler_params=pltpu.CompilerParams(
                collective_id=0, has_side_effects=True, vmem_limit_bytes=67043328),
        )(lengths, freqs, attn_gain, ffn_gain, hidden, k_cache, v_cache, w_q, w_kv, w_o, w_gate, w_up, w_down)

    return jax.shard_map(device_fn, mesh=mesh, in_specs=in_specs, out_specs=out_specs, check_vma=False)
```

```python
import functools

import jax
import jax.numpy as jnp
import numpy as np
from jax import lax
from jax.experimental import pallas as pl
from jax.experimental.pallas import tpu as pltpu
from jax.sharding import PartitionSpec as P

EPS = 1e-5
ROPE_BASE = 10000.0
MESH = pl.DeviceIdType.MESH
F32 = jnp.float32
BF16 = jnp.bfloat16

TN = 256
NS = 16
GS = 8
GU = 7
GU_EARLY = 2
LATE_STEPS = (2, 3, 3, 3, 3)
DN_STEPS = (2, 2, 2, 2, 2, 2, 2)
QKV_STEPS = (4, 5)
O_STEPS = (2, 2, 3)


def spans(steps, total):
    assert sum(steps) == total
    out, at = [], 0
    for n in steps:
        out.append(list(range(at, at + n)))
        at += n
    return out


def dot(lhs, rhs):
    return jnp.dot(lhs, rhs, preferred_element_type=F32)


def kernel(dims, len_ref, freq_ref, ag_ref, fg_ref, hid, kc, vc, wq, wkv, wo, wg, wu, wd, out,
           ring, xc, x1, h, qf, kn, vn, p_s, tot_s, self_s, of, oa, acc_s, u, yp, dr, yr, kb, vb, cos_t, sin_t, len_t,
           ring_sem, cache_sem, in_sem, o_send, o_recv, xp_send, xp_recv, xy_send, xy_recv, xf_send, xf_recv,
           d_send, d_recv, y_send, y_recv, e_send, e_recv):
    n_layers, d_model, ff, heads, kv_heads, head, seq = dims
    half_d = d_model // 2
    nch = d_model // TN
    nq = half_d // TN
    hr = xc.shape[3]
    ngu = ff // 128
    group = heads // kv_heads
    r_o = nq + 2
    r_gu = r_o + nq
    r_dn = r_gu + ngu
    tiles = r_dn + nch
    assert r_gu == NS

    side = lax.axis_index("side")
    dev = lax.axis_index("dev")
    c = lax.rem(side, 2)
    oc = 1 - c
    base = (side - c) * (2 * hr)
    pair = {"side": side + 1 - 2 * c}
    ypeer = {"dev": 1 - dev}

    barrier = pltpu.get_barrier_semaphore()
    pl.semaphore_signal(barrier, inc=1, device_id=pair, device_id_type=MESH)
    pl.semaphore_signal(barrier, inc=1, device_id=ypeer, device_id_type=MESH)

    def rcopy(src, dst, ssem, rsem, where):
        return pltpu.make_async_remote_copy(
            src_ref=src, dst_ref=dst, send_sem=ssem, recv_sem=rsem, device_id=where, device_id_type=MESH)

    def al(v, m):
        return pl.multiple_of(v, m)

    def slot_of(layer, r):
        return lax.rem(layer * tiles + r, NS)

    def fill_attn(layer, r):
        slot = slot_of(layer, r)
        top = ring.at[slot, pl.ds(0, d_model)]
        if r < nq:
            src = wq.at[layer, :, pl.ds(al(c * half_d + r * TN, TN), TN)]
        elif r < r_o:
            src = wkv.at[layer, :, pl.ds(al((r - nq) * (2 * TN) + c * TN, TN), TN)]
        else:
            src = wo.at[layer, :, pl.ds(al(c * half_d + (r - r_o) * TN, TN), TN)]
        pltpu.make_async_copy(src, top, ring_sem.at[slot]).start()

    def fill_gu(layer, i):
        slot = slot_of(layer, r_gu + i)
        col = al(c * ff + i * 128, 128)
        for k, w in enumerate((wg, wu)):
            pltpu.make_async_copy(
                w.at[layer, :, pl.ds(col, 128)], ring.at[slot, pl.ds(0, d_model), pl.ds(k * 128, 128)],
                ring_sem.at[slot]).start()

    def fill_dn(layer, j):
        slot = slot_of(layer, r_dn + j)
        pltpu.make_async_copy(
            wd.at[layer, pl.ds(al(c * ff, 128), ff), pl.ds(al(j * TN, TN), TN)], ring.at[slot], ring_sem.at[slot]).start()

    def wait_top(slot):
        pltpu.make_async_copy(wq.at[0, :, pl.ds(0, TN)], ring.at[slot, pl.ds(0, d_model)], ring_sem.at[slot]).wait()

    def wait_full(slot):
        pltpu.make_async_copy(wd.at[0, pl.ds(0, ff), pl.ds(0, TN)], ring.at[slot], ring_sem.at[slot]).wait()

    def cache_copies(layer, half, core):
        src = pl.ds(al(base + core * (2 * hr) + half * hr, hr), hr)
        hd = pl.ds(c * 2, 2)
        return (pltpu.make_async_copy(kc.at[layer, src, hd], kb.at[core], cache_sem.at[core, 0]),
                pltpu.make_async_copy(vc.at[layer, src, hd], vb.at[core], cache_sem.at[core, 1]))

    def norm_half(read, gain, layer, dst_row):
        for k in range(2):
            total = jnp.zeros((hr, TN), F32)
            for j in range(nch):
                v = read(j, k).astype(F32)
                total = total + v * v
            inv = lax.rsqrt(jnp.sum(total, axis=-1, keepdims=True) * (1.0 / d_model) + EPS)
            r0 = dst_row + k * hr
            for j in range(nch):
                v = read(j, k).astype(F32)
                g = gain[pl.ds(layer, 1), j * TN:(j + 1) * TN]
                h[r0:r0 + hr, j * TN:(j + 1) * TN] = (v * inv * g).astype(BF16)

    def row_copy(j, half, k):
        src = hid.at[pl.ds(al(base + (k * 2 + half) * hr, hr), hr), pl.ds(j * TN, TN)]
        return pltpu.make_async_copy(src, xc.at[j, half, k], in_sem.at[j, half, k])

    rows_in = [[(j, half, k) for j in range(nch) for k in range(2)] for half in range(2)]
    for jhk in rows_in[0]:
        row_copy(*jhk).start()
    for r in range(4):
        fill_attn(0, r)

    n_pos = 4 * hr
    lens = len_ref[pl.ds(lax.div(side, 2), 1), :].astype(F32)
    len_t[...] = jnp.broadcast_to(lens, (n_pos, n_pos)).T
    angle = len_t[:, :head] * freq_ref[...]
    lane = lax.broadcasted_iota(jnp.int32, (n_pos, head), 1)
    cos_t[...] = jnp.cos(angle)
    sin_t[...] = jnp.sin(angle) * jnp.where(lane < head // 2, -1.0, 1.0)

    for jhk in rows_in[0]:
        row_copy(*jhk).wait()
    for r in range(4, r_o):
        fill_attn(0, r)
    for core in range(2):
        for cp in cache_copies(0, 0, core):
            cp.start()
    for jhk in rows_in[1]:
        row_copy(*jhk).start()
    for r in range(r_o, r_gu):
        fill_attn(0, r)
    pl.semaphore_wait(barrier, 2)

    col = lax.broadcasted_iota(jnp.int32, (GS, GS * seq), 1)
    row = lax.broadcasted_iota(jnp.int32, (GS, GS * seq), 0)
    own_keys = lax.shift_right_logical(col, seq.bit_length() - 1) == row
    key_pos = jnp.bitwise_and(col, seq - 1).astype(F32)
    masked = jnp.where(own_keys, -1e30, -jnp.inf)
    scale = head ** -0.5

    def e_copy(half, j, core):
        return rcopy(xc.at[j, half, core], xc.at[j, half, core], e_send.at[half, j], e_recv.at[half, j], pair)

    def out_copy(half, j):
        dst = out.at[pl.ds(half * hr, hr), pl.ds(al(j * TN, TN), TN)]
        return pltpu.make_async_copy(xc.at[j, half, c], dst, e_send.at[half, j])

    def y_copy(half, j):
        return rcopy(yp.at[j, c, half, 1], yr.at[half, j], y_send.at[half, j], y_recv.at[half, j], ypeer)

    def d_copy(j):
        return rcopy(yp.at[j, oc], dr.at[j], d_send.at[j], d_recv.at[j], pair)

    def finish(half, after):
        def one(j, carry):
            y_copy(half, j).wait_recv()
            y = (yp[j, c, half, 0] + dr[j, half, 0] + yr[half, j]).astype(BF16).astype(F32)
            xc[j, half, c] = (x1[0, j, half, c].astype(F32) + y).astype(BF16)
            after(j)
            return carry

        lax.fori_loop(0, nch, one, 0)

    def exchange(half):
        finish(half, lambda j: e_copy(half, j, c).start())
        for j in range(nch):
            e_copy(half, j, oc).wait_recv()
            e_copy(half, j, c).wait_send()

    def sums_sent():
        for j in range(nch):
            d_copy(j).wait_send()
            for half in range(2):
                y_copy(half, j).wait_send()

    def xy_copy(half, j):
        mine = c * nq + j
        return rcopy(x1.at[0, mine, half], x1.at[1, mine, half], xy_send.at[half, j], xy_recv.at[half, j], ypeer)

    def xp_copy(half, j, core):
        at = x1.at[0, core * nq + j, half]
        return rcopy(at, at, xp_send.at[half, j], xp_recv.at[half, j], pair)

    def xf_copy(half, j, core):
        at = x1.at[1, core * nq + j, half]
        return rcopy(at, at, xf_send.at[half, j], xf_recv.at[half, j], pair)

    def o_copy(half, core, cc):
        at = oa.at[cc, half, pl.ds(al(core * hr, hr), hr)]
        return rcopy(at, at, o_send.at[half, core], o_recv.at[half, core], pair)

    def attention_half(layer, half):
        first = half == 0

        def arrive(rs):
            @pl.when(first)
            def _():
                for r in rs:
                    wait_top(slot_of(layer, r))

        def refill(rs):
            @pl.when(jnp.logical_not(first))
            def _():
                for r in rs:
                    fill_gu(layer, r)

        with jax.named_scope("norm_a"):
            norm_half(lambda j, k: xc[j, half, k], ag_ref, layer, 0)

        def both_cores(table):
            return jnp.concatenate([table[pl.ds(al((k * 2 + half) * hr, hr), hr), :] for k in range(2)], axis=0)

        cos_v = both_cores(cos_t)
        sin_v = both_cores(sin_t)

        def rope(v):
            return (v * cos_v + pltpu.roll(v, head // 2, 1) * sin_v).astype(BF16).astype(F32)

        def qkv(r):
            y = dot(h[:2 * hr, :], ring[slot_of(layer, r), :d_model, :])
            for k in range(2):
                part = y[:, k * head:(k + 1) * head]
                if r < nq:
                    qf[r * 2 + k] = rope(part)
                elif r == nq:
                    kn[k] = rope(part)
                else:
                    vn[k] = part.astype(BF16).astype(F32)

        with jax.named_scope("qkv"):
            for rs in spans(QKV_STEPS, r_o):
                arrive(rs)
                for r in rs:
                    qkv(r)
                refill(rs)

        def core_body(core, carry):
            for cp in cache_copies(layer, half, core):
                cp.wait()
            @pl.when(core >= 0)
            def _():
                for gi in range(hr // GS):
                    n_old = len_t[pl.ds(al((core * 2 + half) * hr + gi * GS, GS), GS), :head]
                    n_old = jnp.concatenate([n_old] * (GS * seq // head), axis=1)
                    valid = own_keys & (key_pos < n_old)
                    r0 = al(core * hr + gi * GS, GS)
                    for k in range(2):
                        q = qf[k * group:(k + 1) * group, pl.ds(r0, GS), :]
                        keys = kb[core, gi * GS:(gi + 1) * GS, k].reshape(GS * seq, head)
                        sc = lax.dot_general(q.reshape(group * GS, head).astype(BF16), keys, (((1,), (1,)), ((), ())),
                                             preferred_element_type=F32)
                        sc = sc.reshape(group, GS, GS * seq) * scale
                        sc = jnp.where(valid[None], sc, masked[None])
                        k_new = kn[k, pl.ds(r0, GS), :]
                        self_sc = jnp.sum(q * k_new[None], axis=-1, keepdims=True) * scale
                        top = jnp.maximum(jnp.max(sc, axis=-1, keepdims=True), self_sc)
                        e = jnp.exp(sc - top)
                        self_e = jnp.exp(self_sc - top)
                        total = jnp.sum(e, axis=-1, keepdims=True) + self_e
                        p_s[gi, k] = e.reshape(group * GS, GS * seq).astype(BF16)
                        tot_s[gi, k] = jnp.broadcast_to(total, (group, GS, head))
                        self_s[gi, k] = jnp.broadcast_to(self_e, (group, GS, head))

            @pl.when(core >= 0)
            def _():
                for gi in range(hr // GS):
                    r0 = al(core * hr + gi * GS, GS)
                    for k in range(2):
                        vals = vb[core, gi * GS:(gi + 1) * GS, k].reshape(GS * seq, head)
                        mix = dot(p_s[gi, k], vals).reshape(group, GS, head)
                        mix = mix + self_s[gi, k].astype(BF16).astype(F32) * vn[k, pl.ds(r0, GS), :][None]
                        of[k * group:(k + 1) * group, gi * GS:(gi + 1) * GS, :] = mix / tot_s[gi, k]

            for hh in range(heads // 2):
                oa[c, half, pl.ds(al(core * hr, hr), hr), hh * head:(hh + 1) * head] = of[hh].astype(BF16)
            o_copy(half, core, c).start()

            @pl.when(first)
            def _():
                for cp in cache_copies(layer, 1, core):
                    cp.start()

            @pl.when(jnp.logical_not(first) & (layer + 1 < n_layers))
            def _():
                for cp in cache_copies(layer + 1, 0, core):
                    cp.start()

            return carry

        with jax.named_scope("attn"):
            lax.fori_loop(0, 2, core_body, 0)

        with jax.named_scope("w_o_own"):
            arrive(range(r_o, r_gu))
            for i in range(nq):
                w = ring[slot_of(layer, r_o + i), pl.ds(al(c * half_d, half_d), half_d), :]
                acc_s[i] = dot(oa[c, half], w) + xc[c * nq + i, half].reshape(2 * hr, TN).astype(F32)
        with jax.named_scope("o_wait"):
            @pl.when(jnp.logical_not(first))
            def _():
                for j in range(nq):
                    xy_copy(0, j).wait_recv()
                    xf_copy(0, j, c).start()

            for core in range(2):
                o_copy(half, core, oc).wait_recv()
        with jax.named_scope("w_o"):
            for js in spans(O_STEPS, nq):
                for i in js:
                    w = ring[slot_of(layer, r_o + i), pl.ds(al(oc * half_d, half_d), half_d), :]
                    acc = acc_s[i] + dot(oa[oc, half], w)
                    x1[0, c * nq + i, half] = acc.astype(BF16).reshape(2, hr, TN)
                for i in js:
                    xy_copy(half, i).start()
                    xp_copy(half, i, c).start()
                refill([r_o + i for i in js])

    def layer_body(layer, carry):
        not_last = layer + 1 < n_layers

        def half_body(half, carry):
            @pl.when((half == 1) & (layer == 0))
            def _():
                for jhk in rows_in[1]:
                    row_copy(*jhk).wait()

            @pl.when((half == 1) & (layer > 0))
            def _():
                with jax.named_scope("finish_b"):
                    exchange(1)
                    sums_sent()

            attention_half(layer, half)
            return carry

        lax.fori_loop(0, 2, half_body, 0)

        def norm_f(chip, half):
            read = lambda j, k: x1[chip, j, half, k]
            norm_half(read, fg_ref, layer, (chip * 2 + half) * 2 * hr)

        with jax.named_scope("ag_first"):
            for j in range(nq):
                xp_copy(0, j, oc).wait_recv()
            norm_f(0, 0)
            for j in range(nq):
                xf_copy(0, j, oc).wait_recv()
            norm_f(1, 0)
            for j in range(nq):
                xp_copy(1, j, oc).wait_recv()
            norm_f(0, 1)

        def gate_up(first, count, r0, r1, wait, fill):
            slots = [slot_of(layer, r_gu + first + i) for i in range(count)]
            if wait:
                for slot in slots:
                    wait_top(slot)
            for i, slot in enumerate(slots):
                y = dot(h[r0:r1, :], ring[slot, :d_model, :])
                gate = y[:, :128]
                act = gate * (1.0 / (1.0 + jnp.exp(-gate))) * y[:, 128:]
                u[r0:r1, pl.ds(al((first + i) * 128, 128), 128)] = act.astype(BF16)
            if fill:
                for i in range(count):
                    fill(first + i)

        n_a = ngu - NS
        n_b = nch
        n_rows = 8 * hr
        late = 6 * hr
        assert n_b % GU == 0 and GU_EARLY * GU < NS < n_a

        def gu_early(i, carry):
            gate_up(i * GU, GU, 0, late, True, None)

            def forward(j, carry):
                xy_copy(1, j).wait_recv()
                xf_copy(1, j, c).start()
                return carry

            lax.fori_loop(nq * i // GU_EARLY, nq * (i + 1) // GU_EARLY, forward, 0)
            return carry

        def fill_a(t):
            fill_gu(layer, t + NS)

        def gu_b(i, carry):
            gate_up(n_a + i * GU, GU, 0, n_rows, True, lambda t: fill_dn(layer, t - n_a))
            return carry

        def fill_next(t):
            @pl.when(not_last)
            def _():
                fill_attn(layer + 1, t - n_a - n_b)

        with jax.named_scope("gu_early"):
            lax.fori_loop(0, GU_EARLY, gu_early, 0)
        with jax.named_scope("ag_last"):
            for j in range(nq):
                xf_copy(1, j, oc).wait_recv()
            norm_f(1, 1)
        with jax.named_scope("gu_late"):
            for ts in spans(LATE_STEPS, GU_EARLY * GU):
                gate_up(ts[0], len(ts), late, n_rows, False, fill_a)
        with jax.named_scope("gate_up"):
            gate_up(GU_EARLY * GU, NS - GU_EARLY * GU, 0, n_rows, True, fill_a)
            gate_up(NS, n_a - NS, 0, n_rows, True, fill_a)
            lax.fori_loop(0, n_b // GU, gu_b, 0)
            gate_up(n_a + n_b, ngu - n_a - n_b, 0, n_rows, True, fill_next)

        for half in range(2):
            for j in range(nq):
                xf_copy(half, j, c).wait_send()
                xy_copy(half, j).wait_send()
                xp_copy(half, j, c).wait_send()
            for core in range(2):
                o_copy(half, core, c).wait_send()

        def pair_sum(j):
            d_copy(j).wait_recv()
            for half in range(2):
                yp[j, c, half, 1] = yp[j, c, half, 1] + dr[j, half, 1]
            y_copy(0, j).start()

        def down(js, before):
            slots = [slot_of(layer, r_dn + j) for j in js]
            for slot in slots:
                wait_full(slot)
            for j, slot in zip(js, slots):
                y = dot(u[...], ring[slot])
                for chip in range(2):
                    for half in range(2):
                        for core in range(2):
                            r0 = ((chip * 2 + half) * 2 + core) * hr
                            yp[j, core, half, chip] = y[r0:r0 + hr, :]
            for j in js:
                d_copy(j).start()

            @pl.when(not_last)
            def _():
                for j in js:
                    fill_attn(layer + 1, j + ngu - n_a - n_b)

            for j in before:
                pair_sum(j)

        with jax.named_scope("down"):
            steps = spans(DN_STEPS, nch)
            for js, before in zip(steps, [[]] + steps[:-1]):
                down(js, before)
        with jax.named_scope("pair_last"):
            for j in steps[-1]:
                pair_sum(j)
            for j in range(nch):
                y_copy(1, j).start()

        with jax.named_scope("finish_a"):
            @pl.when(not_last)
            def _():
                exchange(0)

            @pl.when(jnp.logical_not(not_last))
            def _():
                finish(0, lambda j: out_copy(0, j).start())

        return carry

    lax.fori_loop(0, n_layers, layer_body, 0)
    with jax.named_scope("finish_b"):
        finish(1, lambda j: out_copy(1, j).start())
        sums_sent()
        for half in range(2):
            for j in range(nch):
                out_copy(half, j).wait()


def solution(mesh):
    batch_axes = ('inst', 'dev')
    in_specs = (
        P(batch_axes, None),
        P(batch_axes),
        P(None, batch_axes, None, None, None),
        P(None, batch_axes, None, None, None),
        P(), P(), P(), P(), P(),
        P(None, None, 'dev'),
        P(None, None, 'dev'),
        P(None, 'dev', None),
    )
    out_specs = P(('inst', 'dev', 'side'), None)
    n_side = mesh.shape['side']

    def device_fn(hidden, cache_len, k_cache, v_cache, w_q, w_kv, w_o, attn_gain, ffn_gain, w_gate, w_up, w_down):
        n_layers, d_model, _ = w_q.shape
        kv_heads, seq, head = k_cache.shape[2:]
        heads = w_q.shape[2] // head
        rows = hidden.shape[0] // n_side
        ff = w_gate.shape[2] // 2
        nch = d_model // TN
        nq = nch // 2
        hr = rows // 2
        group = heads // kv_heads
        half_dim = head // 2
        freqs = np.float32(ROPE_BASE) ** (-np.arange(half_dim, dtype=np.float32) / np.float32(half_dim))
        freqs = jnp.asarray(np.concatenate([freqs, freqs])[None].astype(np.float32))
        lengths = cache_len.reshape(n_side // 2, 2 * rows)
        dims = (n_layers, d_model, ff, heads, kv_heads, head, seq)
        vmem = pl.BlockSpec(memory_space=pltpu.VMEM)
        hbm = pl.BlockSpec(memory_space=pl.ANY)
        dma = pltpu.SemaphoreType.DMA
        return pl.pallas_call(
            functools.partial(kernel, dims),
            name='decode_layers',
            out_shape=jax.ShapeDtypeStruct((rows, d_model), BF16),
            in_specs=[vmem] * 4 + [hbm] * 9,
            out_specs=hbm,
            scratch_shapes=[
                pltpu.VMEM((NS, ff, TN), BF16),
                pltpu.VMEM((nch, 2, 2, hr, TN), BF16),
                pltpu.VMEM((2, nch, 2, 2, hr, TN), BF16),
                pltpu.VMEM((4 * rows, d_model), BF16),
                pltpu.VMEM((heads // 2, rows, head), F32),
                pltpu.VMEM((2, rows, head), F32),
                pltpu.VMEM((2, rows, head), F32),
                pltpu.VMEM((hr // GS, 2, group * GS, GS * seq), BF16),
                pltpu.VMEM((hr // GS, 2, group, GS, head), F32),
                pltpu.VMEM((hr // GS, 2, group, GS, head), F32),
                pltpu.VMEM((heads // 2, hr, head), F32),
                pltpu.VMEM((2, 2, rows, d_model // 2), BF16),
                pltpu.VMEM((nq, rows, TN), F32),
                pltpu.VMEM((4 * rows, ff), BF16),
                pltpu.VMEM((nch, 2, 2, 2, hr, TN), F32),
                pltpu.VMEM((nch, 2, 2, hr, TN), F32),
                pltpu.VMEM((2, nch, hr, TN), F32),
                pltpu.VMEM((2, hr, 2, seq, head), BF16),
                pltpu.VMEM((2, hr, 2, seq, head), BF16),
                pltpu.VMEM((2 * rows, head), F32),
                pltpu.VMEM((2 * rows, head), F32),
                pltpu.VMEM((2 * rows, 2 * rows), F32),
                dma((NS,)), dma((2, 2)), dma((nch, 2, 2)),
                dma((2, 2)), dma((2, 2)),
                dma((2, nq)), dma((2, nq)), dma((2, nq)), dma((2, nq)), dma((2, nq)), dma((2, nq)),
                dma((nch,)), dma((nch,)), dma((2, nch)), dma((2, nch)), dma((2, nch)), dma((2, nch)),
            ],
            compiler_params=pltpu.CompilerParams(
                collective_id=0, has_side_effects=True, vmem_limit_bytes=67043328),
        )(lengths, freqs, attn_gain, ffn_gain, hidden, k_cache, v_cache, w_q, w_kv, w_o, w_gate, w_up, w_down)

    return jax.shard_map(device_fn, mesh=mesh, in_specs=in_specs, out_specs=out_specs, check_vma=False)
```
